32 devices in a mesh: wide: 4 (over x, core), narrow: 8 (over z, y).
Axes of the slice: x: 2, y: 2, z: 4, core: 2. Of those that a mesh axis runs over, the one named last changes fastest.
Arguments:
- inputs: bfloat16 [16384, 1024], P(('wide', 'narrow')), may hold values from -6 to 6
- w_first: bfloat16 [1024, 1024], replicated, may hold values from -0.1875 to 0.1875
- w_second: bfloat16 [1024, 256], replicated, may hold values from -0.1875 to 0.1875
- requests: int32 [128, 128], P(('wide', 'narrow')), may hold values from 0 to 511
- slots: int32 [16384, 15], P(('wide', 'narrow')), may hold values from 0 to 511
- counts: int32 [16384], P(('wide', 'narrow')), may hold values from 1 to 15
- edge_weight: int32 [16384, 15], P(('wide', 'narrow')), may hold values from 1 to 4
- offsets: int32 [4], replicated, may hold values from 0 to 511
Outputs:
- grad_first: float32 [1024, 1024], P('wide')
- grad_second: float32 [1024, 256], P('wide')
The draws below stay inside these ranges and needn't reach their ends.
Inputs may be any that keep to these rules, and one draw needn't show every extreme that they name: requests of block d only name rows of blocks with the same narrow index as d.
All inputs are finite; a program needn't handle non-finite values.
Results may differ from the reference program's by a relative error of at most 0.0018.
Values may be sent and summed in bfloat16 or wider, within the bound.
No kernel may reach another device: no remote copies, remote signals or barrier semaphores. Data moves between devices by JAX's collectives and lax.ppermute only.
A program may use at most 64 MiB of HBM per device.

```python
import math
import jax
import jax.numpy as jnp
from jax import lax

ROWS = 512
DIN = 1024
HID = 1024
E = 256
K = 15
SHIFTS = 4
NEGW = 8
CAP = 128
ROWS_ALL = 16384
N_WIDE = 4
N_NARROW = 8


def plant(result, stream_key, low, largest):
    shape = result.shape
    spot = [jax.random.randint(jax.random.fold_in(stream_key, axis), (), 0, shape[axis]) for axis in range(len(shape))]
    result = result.at[tuple(spot)].set(low)
    longest = shape.index(max(shape))
    spot[longest] = (spot[longest] + 1) % shape[longest]
    return result.at[tuple(spot)].set(largest)


def raised(entries, stream_key, source, target, shards_of, factor):
    owner, partner = [(jnp.arange(entries.shape[position]) // (entries.shape[position] // shards_of)).reshape([-1 if axis == position else 1 for axis in range(entries.ndim)]) for position in (source, target)]
    chosen = jax.random.permutation(stream_key, shards_of)[partner]
    strong = (owner == chosen) | (owner == (partner + shards_of // 2) % shards_of)
    return jnp.where(strong, factor * entries, entries)


def block_scale(stream_key, extent, pieces, low, largest):
    level = 1.0
    for position, blocks in pieces:
        steps = jax.random.uniform(jax.random.fold_in(jax.random.fold_in(stream_key, 6), position), (blocks,), jnp.float32, low / len(pieces), largest / len(pieces))
        level = level * jnp.repeat(jnp.exp(steps), extent[position] // blocks).reshape((-1,) + (1,) * (len(extent) - 1 - position))
    return level


def noise(stream_key, extent, deviation, bound, shards=(), held_as=jnp.bfloat16):
    loudness = block_scale(stream_key, extent, shards, -0.22, 0.18) if shards else 1.0
    array = jax.random.normal(stream_key, extent, jnp.float32) * deviation * loudness
    return jnp.minimum(jnp.maximum(array, -bound), bound).astype(held_as)


def bell_draw_with(key, extent, width, most, shards, heavy, held_as=jnp.bfloat16):
    drawn = width * jax.random.normal(key, extent, jnp.float32)
    if shards:
        drawn = drawn * block_scale(key, extent, shards, -0.22, 0.18)
    return jnp.clip(raised(drawn, jax.random.fold_in(key, 3), *heavy), -most, most).astype(held_as)


def setup_inputs(seed: int = 0) -> dict:
    arg_keys = jax.random.split(jax.random.key(seed), 9)
    return {
        "inputs": bell_draw_with(arg_keys[0], (ROWS_ALL, DIN), 1.0, 6.0, ((0, 32),), (0, 1, 32, 2.75)),
        "w_first": noise(arg_keys[1], (DIN, HID), DIN ** -0.5, 0.1875),
        "w_second": noise(arg_keys[2], (HID, E), HID ** -0.5, 0.1875),
        "requests": plant(jax.random.randint(arg_keys[3], (N_WIDE * N_NARROW * N_WIDE, CAP), 0, ROWS), jax.random.fold_in(arg_keys[3], 1), 0, ROWS - 1).astype(jnp.int32),
        "slots": plant(jax.random.randint(arg_keys[4], (ROWS_ALL, K), 0, N_WIDE * CAP), jax.random.fold_in(arg_keys[4], 1), 0, (N_WIDE * CAP) - 1).astype(jnp.int32),
        "counts": plant(jax.random.randint(arg_keys[5], (ROWS_ALL,), 1, K + 1), jax.random.fold_in(arg_keys[5], 1), 1, K).astype(jnp.int32),
        "edge_weight": plant(jax.random.randint(arg_keys[6], (ROWS_ALL, K), 1, 5), jax.random.fold_in(arg_keys[6], 1), 1, 4).astype(jnp.int32),
        "offsets": plant(jax.random.randint(arg_keys[7], (SHIFTS,), 0, ROWS), jax.random.fold_in(arg_keys[7], 1), 0, ROWS - 1).astype(jnp.int32),
    }


def forward(block, w_first, w_second):
    pre = jnp.dot(block, w_first, preferred_element_type=jnp.float32)
    hidden = jnp.maximum(pre, 0.0).astype(jnp.bfloat16)
    codes = jnp.dot(hidden, w_second, preferred_element_type=jnp.float32)
    return (pre, hidden, codes)

def attract(codes, near, weight):
    diff = codes[:, None, :] - near.astype(jnp.float32)
    dist = lax.optimization_barrier(jnp.sum(diff * diff, axis=-1)) / diff.shape[-1]
    return lax.optimization_barrier(jnp.sum((weight / (1.0 + dist))[:, :, None] * diff, axis=1))

def repel(codes, far):
    diff = codes[:, None, :] - far.astype(jnp.float32)
    dist = lax.optimization_barrier(jnp.sum(diff * diff, axis=-1)) / diff.shape[-1]
    onep = 1.0 + dist
    coef = 1.0 / (onep * onep * (dist / onep + 0.1))
    return -lax.optimization_barrier(jnp.sum(coef[:, :, None] * diff, axis=1))

def negatives(block, offset, count):
    rows = block.shape[0]
    index = (jnp.arange(rows, dtype=jnp.int32)[:, None] + offset + jnp.arange(count, dtype=jnp.int32)[None, :]) % rows
    return block[index]

def reference(inputs, w_first, w_second, requests, slots, counts, edge_weight, offsets):
    devices = N_WIDE * N_NARROW
    blocks = inputs.reshape(devices, ROWS, DIN)

    def encode(block):
        return forward(block, w_first, w_second)[2].astype(jnp.bfloat16)
    sent = lax.map(encode, blocks)
    asked = requests.reshape(devices, N_WIDE, CAP)
    near_slots = slots.reshape(devices, ROWS, K)
    near_counts = counts.reshape(devices, ROWS)
    near_weight = edge_weight.reshape(devices, ROWS, K)
    scale = 2.0 / (K * math.sqrt(ROWS_ALL))

    def accumulate(carry, index):
        wide_idx = index // N_NARROW
        narrow_idx = index % N_NARROW
        pre, hidden, codes = forward(blocks[index], w_first, w_second)
        owners = jnp.arange(N_WIDE, dtype=jnp.int32) * N_NARROW + narrow_idx
        table = sent[owners[:, None], asked[index]].reshape(N_WIDE * CAP, E)
        near = table[near_slots[index]]
        live = jnp.arange(K, dtype=jnp.int32)[None, :] < near_counts[index][:, None]
        weight = jnp.where(live, near_weight[index].astype(jnp.float32), jnp.float32(0.0))
        grad = attract(codes, near, weight)
        for step in range(SHIFTS):
            source = wide_idx * N_NARROW + (narrow_idx - step - 1) % N_NARROW
            grad = grad + repel(codes, negatives(sent[source], offsets[step], NEGW))
        dcodes = (scale * grad).astype(jnp.bfloat16)
        part_second = jnp.dot(hidden.T, dcodes, preferred_element_type=jnp.float32)
        dhidden = jnp.dot(dcodes, w_second.T, preferred_element_type=jnp.float32)
        dpre = jnp.where(pre > 0, dhidden, jnp.float32(0.0)).astype(jnp.bfloat16)
        part_first = jnp.dot(blocks[index].T, dpre, preferred_element_type=jnp.float32)
        return ((carry[0] + part_first, carry[1] + part_second), None)
    start = (jnp.zeros((DIN, HID), jnp.float32), jnp.zeros((HID, E), jnp.float32))
    (grad_first, grad_second), _ = lax.scan(accumulate, start, jnp.arange(devices, dtype=jnp.int32))
    return (grad_first, grad_second)
```

```python
import functools
import math

import jax
import jax.numpy as jnp
from jax import lax
from jax.experimental import pallas as pl
from jax.experimental.pallas import tpu as pltpu
from jax.sharding import PartitionSpec as P

NEGW = 8
LANES = 128
HALF = LANES // 2
FULL = 32000.0
STEPS = 128.0
TINY = 1e-30

F32 = jnp.float32
BF16 = jnp.bfloat16
I16 = jnp.int16
VMEM = pl.BlockSpec(memory_space=pltpu.VMEM)
SMEM = pl.BlockSpec(memory_space=pltpu.SMEM)


def call(body, out_shape, n_scalars, n_arrays, scratch=()):
    many = isinstance(out_shape, (list, tuple))
    return pl.pallas_call(
        body,
        out_shape=out_shape,
        in_specs=[SMEM] * n_scalars + [VMEM] * n_arrays,
        out_specs=[VMEM] * len(out_shape) if many else VMEM,
        scratch_shapes=list(scratch),
        compiler_params=pltpu.CompilerParams(vmem_limit_bytes=40 * 1024 * 1024),
    )


def dot(a, b):
    return lax.dot_general(a, b, (((1,), (0,)), ((), ())), preferred_element_type=F32)


def dot_nt(a, b):
    return lax.dot_general(a, b, (((1,), (1,)), ((), ())), preferred_element_type=F32)


def parts(value, count):
    out = []
    for _ in range(count):
        part = value.astype(BF16)
        out.append(part)
        value = value - part.astype(F32)
    return out


def distances(y, z):
    gram = sum(dot_nt(part, z) for part in parts(y, 3))
    zf = z.astype(F32)
    ones = jnp.ones((8, z.shape[1]), BF16)
    z_norm = sum(dot_nt(ones, part) for part in parts(zf * zf, 2))[0:1]
    y_norm = jnp.sum(y * y, axis=1, keepdims=True)
    return jnp.maximum(y_norm + z_norm - 2.0 * gram, 0.0) / z.shape[1]


def pull(y, z, coef):
    high, low = parts(coef, 2)
    total = jnp.sum(high.astype(F32) + low.astype(F32), axis=1, keepdims=True)
    return y * total - (dot(high, z) + dot(low, z))


def near_body(codes, table, slots, counts, edges, inputs, hidden, out, inputs_t, hidden_t):
    y, z = codes[...], table[...]
    column = lax.broadcasted_iota(jnp.int32, (y.shape[0], z.shape[0]), 1)
    weight = jnp.zeros((y.shape[0], z.shape[0]), F32)
    for k in range(slots.shape[1]):
        live = jnp.where(k < counts[...], edges[:, k : k + 1].astype(F32), 0.0)
        weight = weight + jnp.where(column == slots[:, k : k + 1], live, 0.0)
    out[...] = pull(y, z, weight / (1.0 + distances(y, z)))
    inputs_t[...] = inputs[...].T
    hidden_t[...] = hidden[...].T


def repulsion(y, z, offset):
    rows = z.shape[0]
    shape = (y.shape[0], rows)
    place = lax.broadcasted_iota(jnp.int32, shape, 1) - lax.broadcasted_iota(jnp.int32, shape, 0)
    place = place - offset
    place = jnp.where(place < 0, place + rows, place)
    place = jnp.where(place < 0, place + rows, place)
    dist = distances(y, z)
    onep = 1.0 + dist
    coef = jnp.where(place < NEGW, 1.0 / (onep * (dist + 0.1 * onep)), 0.0)
    return pull(y, z, coef)


def far_body(step, offsets, codes, block, grad, out):
    out[...] = grad[...] - repulsion(codes[...], block[...], offsets[step])


def pick_body(asked, sent, out):
    rows = sent.shape[0]
    for p in range(asked.shape[0]):
        hot = lax.broadcasted_iota(jnp.int32, (rows, asked.shape[1]), 0) == asked[p : p + 1, :]
        hot = jnp.where(hot, 1.0, 0.0).astype(BF16).T
        out[p] = dot(hot, sent[...]).astype(BF16)


def encode(value, first):
    quanta, codes = [], []
    for piece in (value[:, :first], value[:, first:]):
        top = jnp.maximum(jnp.max(jnp.abs(piece), axis=1, keepdims=True), TINY)
        code = jnp.ceil(jnp.log2(top) * STEPS)
        unit = FULL / jnp.exp2(code / STEPS)
        quanta.append(jnp.round(piece * unit))
        codes.append(code)
    lane = lax.broadcasted_iota(jnp.int32, (value.shape[0], LANES), 1)
    quanta.append(jnp.where(lane < HALF, codes[0], codes[1]))
    return [q.astype(jnp.int32).astype(I16) for q in quanta]


def decode(packed, first, width):
    code = packed[:, width:].astype(jnp.int32).astype(F32)
    out = []
    for lane, low, high in ((0, 0, first), (HALF, first, width)):
        unit = jnp.exp2(code[:, lane : lane + 1] / STEPS) / FULL
        out.append(packed[:, low:high].astype(jnp.int32).astype(F32) * unit)
    return out


def put_encoded(ref, value, first):
    width = value.shape[1]
    a, b, c = encode(value, first)
    ref[:, :first] = a
    ref[:, first:width] = b
    ref[:, width:] = c


def gradients(step, scale, offsets, codes, block, grad, w_second, hidden):
    total = grad[...] - repulsion(codes[...], block[...], offsets[step])
    dcodes = (scale * total).astype(BF16)
    dhidden = dot_nt(dcodes, w_second[...])
    dpre = jnp.where(hidden[...] > 0, dhidden, 0.0).astype(BF16)
    return dcodes, dpre


def last_body(step, scale, offsets, bit, codes, block, grad, w_second, hidden, inputs_t, hidden_t, keep, send):
    dcodes, dpre = gradients(step, scale, offsets, codes, block, grad, w_second, hidden)
    first = dpre.shape[1]
    rows = keep.shape[1]
    mine = bit[0]
    for a in range(keep.shape[0]):
        rows_of = pl.ds(pl.multiple_of((2 * a + 1 - mine) * rows, rows), rows)
        piece = jnp.concatenate([dot(inputs_t[rows_of, :], dpre), dot(hidden_t[rows_of, :], dcodes)], axis=1)
        put_encoded(send.at[a], piece, first)
    for a in range(keep.shape[0]):
        rows_of = pl.ds(pl.multiple_of((2 * a + mine) * rows, rows), rows)
        keep[a, :, :first] = dot(inputs_t[rows_of, :], dpre)
        keep[a, :, first:] = dot(hidden_t[rows_of, :], dcodes)


def last_plain_body(step, scale, offsets, codes, block, grad, w_second, hidden, inputs_t, hidden_t, one, two):
    dcodes, dpre = gradients(step, scale, offsets, codes, block, grad, w_second, hidden)
    one[...] = dot(inputs_t[...], dpre)
    two[...] = dot(hidden_t[...], dcodes)


def stage_body(first, bit, held, got, keep, send):
    width = held.shape[3]
    mine = bit[0]
    for a in range(held.shape[0]):
        for ref, index in ((send, 1 - mine), (keep, mine)):
            pieces = decode(got.at[a, index], first, width)
            piece = held[a, index] + jnp.concatenate(pieces, axis=1)
            if ref is send:
                put_encoded(send.at[a], piece, first)
            else:
                keep[a] = piece


def close_body(first, held, got, out):
    width = held.shape[1]
    put_encoded(out, held[...] + jnp.concatenate(decode(got, first, width), axis=1), first)


def spread_body(first, me, *refs):
    one, two = refs[-2:]
    rows = refs[0].shape[1]
    width = first + two.shape[1]
    place = 0
    for ref in refs[:-2]:
        for j in range(ref.shape[0]):
            at = pl.ds(pl.multiple_of((me[0] ^ place) * rows, rows), rows)
            one[at, :], two[at, :] = decode(ref.at[j], first, width)
            place += 1


def from_behind(block, axis, distance):
    devices = range(lax.axis_size(axis))
    route = [((i - distance) % len(devices), i) for i in devices]
    return lax.ppermute(block, axis, route)


def swapped(block, axis, bit):
    return lax.ppermute(block, axis, [(i, i ^ bit) for i in range(lax.axis_size(axis))])


def bits(count):
    return [1 << b for b in range(count.bit_length() - 1)]


def shards(inputs, w_first, w_second, requests, slots, counts, edge_weight, offsets):
    rows = inputs.shape[0]
    width = w_second.shape[1]
    peers = lax.axis_size("wide")
    group = lax.axis_size("narrow")
    din, hid = w_first.shape
    total_rows = rows * peers * group
    asked = lax.all_to_all(requests, "wide", split_axis=0, concat_axis=0, tiled=True)
    pre = jnp.dot(inputs, w_first, preferred_element_type=F32)
    hidden = jnp.maximum(pre, 0.0).astype(BF16)
    codes = jnp.dot(hidden, w_second, preferred_element_type=F32)
    sent = codes.astype(BF16)
    steps = offsets.shape[0]
    blocks = []
    for step in range(steps):
        blocks.append(from_behind(sent if step < 2 else blocks[step - 2], "narrow", min(step, 1) + 1))
    found = call(pick_body, jax.ShapeDtypeStruct(asked.shape + (width,), BF16), 0, 2)(asked, sent)
    table = lax.all_to_all(found, "wide", split_axis=0, concat_axis=0, tiled=True).reshape(-1, width)
    like = functools.partial(jax.ShapeDtypeStruct, codes.shape, F32)
    grad, inputs_t, hidden_t = call(
        near_body,
        (
            like(),
            jax.ShapeDtypeStruct((din, rows), BF16),
            jax.ShapeDtypeStruct((hid, rows), BF16),
        ),
        0,
        7,
    )(codes, table, slots, counts[:, None], edge_weight, inputs, hidden)
    for step in range(steps - 1):
        grad = call(functools.partial(far_body, step), like(), 1, 3)(offsets, codes, blocks[step], grad)
    scale = 2.0 / (slots.shape[1] * math.sqrt(total_rows))
    wide, narrow = lax.axis_index("wide"), lax.axis_index("narrow")
    chunk = din // (peers * group)
    powers = peers & (peers - 1) == 0 and group & (group - 1) == 0 and peers > 1 and group > 1
    if din != hid or not powers or chunk % 16 or din % (peers * group):
        one, two = call(
            functools.partial(last_plain_body, steps - 1, scale),
            (jax.ShapeDtypeStruct((din, hid), F32), jax.ShapeDtypeStruct((hid, width), F32)),
            1,
            7,
        )(offsets, codes, blocks[-1], grad, w_second, hidden, inputs_t, hidden_t)
        owned = (
            lax.psum_scatter(one, "wide", scatter_dimension=0, tiled=True),
            lax.psum_scatter(two, "wide", scatter_dimension=0, tiled=True),
        )
        return lax.psum(owned, "narrow")

    first, full = hid, hid + width

    def half(groups, lines):
        return (
            jax.ShapeDtypeStruct((groups, lines, full), F32),
            jax.ShapeDtypeStruct((groups, lines, full + LANES), I16),
        )

    plan = [("wide", bit, peers // (2 * bit), din // peers) for bit in bits(peers)]
    low, *high = bits(group)
    plan.append(("narrow", low, group // 2, chunk))
    plan += [("narrow", bit, 1, chunk * bit // 2) for bit in reversed(high)]

    def side(axis, bit):
        index = wide if axis == "wide" else narrow
        return ((index // bit) % 2).reshape(1).astype(jnp.int32)

    axis, bit, groups, lines = plan[0]
    keep, send = call(functools.partial(last_body, steps - 1, scale), half(groups, lines), 2, 7)(
        offsets, side(axis, bit), codes, blocks[-1], grad, w_second, hidden, inputs_t, hidden_t
    )
    got = swapped(send, axis, bit)
    for axis, bit, groups, lines in plan[1:]:
        keep, send = call(functools.partial(stage_body, first), half(groups, lines), 1, 2)(
            side(axis, bit),
            keep.reshape(groups, 2, lines, full),
            got.reshape(groups, 2, lines, full + LANES),
        )
        got = swapped(send, axis, bit)
    mine = call(
        functools.partial(close_body, first), jax.ShapeDtypeStruct((chunk, full + LANES), I16), 0, 2
    )(keep.reshape(chunk, full), got.reshape(chunk, full + LANES))
    held = {0: mine[None]}
    for bit in high + [low]:
        places = sorted(held)
        moved = swapped(jnp.concatenate([held[p] for p in places]), "narrow", bit)
        held.update({p ^ bit: moved[j : j + 1] for j, p in enumerate(places)})
    return call(
        functools.partial(spread_body, first),
        (
            jax.ShapeDtypeStruct((din // peers, hid), F32),
            jax.ShapeDtypeStruct((hid // peers, width), F32),
        ),
        1,
        1,
    )(narrow.reshape(1).astype(jnp.int32), jnp.concatenate([held[p] for p in range(group)]))


def solution(mesh):
    return jax.shard_map(
        shards,
        mesh=mesh,
        in_specs=(
            P(("wide", "narrow"), None),
            P(),
            P(),
            P(("wide", "narrow"), None),
            P(("wide", "narrow"), None),
            P(("wide", "narrow")),
            P(("wide", "narrow"), None),
            P(),
        ),
        out_specs=(P("wide", None), P("wide", None)),
        check_vma=False,
    )
```

```python
import functools
import math

import jax
import jax.numpy as jnp
from jax import lax
from jax.experimental import pallas as pl
from jax.experimental.pallas import tpu as pltpu
from jax.sharding import PartitionSpec as P

NEGW = 8
TILE = 128
PACK = 16
LANES = 128
HALF = LANES // 2
FULL = 32000.0
STEPS = 128.0
TINY = 1e-30

F32 = jnp.float32
BF16 = jnp.bfloat16
I16 = jnp.int16
VMEM = pl.BlockSpec(memory_space=pltpu.VMEM)
SMEM = pl.BlockSpec(memory_space=pltpu.SMEM)


def call(body, out_shape, n_scalars, n_arrays, scratch=(), mib=16):
    many = isinstance(out_shape, (list, tuple))
    return pl.pallas_call(
        body,
        out_shape=out_shape,
        in_specs=[SMEM] * n_scalars + [VMEM] * n_arrays,
        out_specs=[VMEM] * len(out_shape) if many else VMEM,
        scratch_shapes=list(scratch),
        compiler_params=pltpu.CompilerParams(vmem_limit_bytes=mib * 1024 * 1024),
    )


def dot(a, b):
    return lax.dot_general(a, b, (((1,), (0,)), ((), ())), preferred_element_type=F32)


def dot_nt(a, b):
    return lax.dot_general(a, b, (((1,), (1,)), ((), ())), preferred_element_type=F32)


def parts(value, count):
    out = []
    for _ in range(count):
        part = value.astype(BF16)
        out.append(part)
        value = value - part.astype(F32)
    return out


def norms(z):
    zf = z.astype(F32)
    ones = jnp.ones((8, z.shape[1]), BF16)
    return sum(dot_nt(ones, part) for part in parts(zf * zf, 2))[0:1]


def distances(y, z, z_norm):
    gram = sum(dot_nt(part, z) for part in parts(y, 3))
    y_norm = jnp.sum(y * y, axis=1, keepdims=True)
    return jnp.maximum(y_norm + z_norm - 2.0 * gram, 0.0) * (1.0 / z.shape[1])


def pull(y, z, coef):
    high, low = parts(coef, 2)
    total = jnp.sum(high.astype(F32) + low.astype(F32), axis=1, keepdims=True)
    return y * total - (dot(high, z) + dot(low, z))


def flip_body(inputs, hidden, inputs_t, hidden_t):
    inputs_t[...] = inputs[...].T
    hidden_t[...] = hidden[...].T


def near_body(me, codes, requests, slots, counts, edges, grad, *rest):
    out, table = rest[-2:]
    cap = requests.shape[1]
    place = 0
    for ref in rest[:-2]:
        for j in range(ref.shape[0]):
            rows = ref.shape[1]
            asked = requests[pl.ds(me[0] ^ place, 1), :]
            hot = lax.broadcasted_iota(jnp.int32, (rows, cap), 0) == asked
            hot = jnp.where(hot, 1.0, 0.0).astype(BF16).T
            at = pl.ds(pl.multiple_of((me[0] ^ place) * cap, cap), cap)
            table[at, :] = dot(hot, ref[j]).astype(BF16)
            place += 1
    z = table[...]
    z_norm = norms(z)
    tile = min(codes.shape[0], TILE)
    column = lax.broadcasted_iota(jnp.int32, (tile, z.shape[0]), 1)
    for at in range(0, codes.shape[0], tile):
        rows_of = slice(at, at + tile)
        y = codes[rows_of, :]
        weight = jnp.zeros((tile, z.shape[0]), F32)
        live = lax.broadcasted_iota(jnp.int32, (tile, edges.shape[1]), 1) < counts[rows_of, :]
        live = jnp.where(live, edges[rows_of, :].astype(F32), 0.0)
        for k in range(slots.shape[1]):
            weight = weight + jnp.where(column == slots[rows_of, k : k + 1], live[:, k : k + 1], 0.0)
        out[rows_of, :] = grad[rows_of, :] + pull(y, z, weight / (1.0 + distances(y, z, z_norm)))


def repulsion(codes, block, offset, twice, put):
    rows = block.shape[0]
    tile = min(rows, TILE)
    window = tile + max(tile, LANES)
    for at in range(0, twice.shape[0], rows):
        end = min(rows, twice.shape[0] - at)
        twice[at : at + end, :] = block[:end, :]
    start = (offset // PACK) * PACK
    shape = (tile, window)
    place = lax.broadcasted_iota(jnp.int32, shape, 1) - lax.broadcasted_iota(jnp.int32, shape, 0)
    place = place - (offset - start)
    band = (place >= 0) & (place < NEGW)
    for at in range(0, rows, tile):
        y = codes[at : at + tile, :]
        z = twice[pl.ds(pl.multiple_of(start + at, PACK), window), :]
        dist = distances(y, z, norms(z))
        onep = 1.0 + dist
        coef = jnp.where(band, 1.0 / (onep * (dist + 0.1 * onep)), 0.0)
        put(slice(at, at + tile), pull(y, z, coef))


def twice_of(rows, width):
    tile = min(rows, TILE)
    return pltpu.VMEM((2 * rows + max(tile, LANES), width), BF16)


def far_body(step, started, offsets, codes, block, *rest):
    grad, out, twice = rest if started else (None,) + rest

    def put(at, value):
        out[at, :] = grad[at, :] - value if started else -value

    repulsion(codes, block, offsets[step], twice, put)


def encode(one, two):
    quanta, codes = [], []
    for piece in (one, two):
        top = jnp.maximum(jnp.max(jnp.abs(piece), axis=1, keepdims=True), TINY)
        code = jnp.ceil(jnp.log2(top) * STEPS)
        unit = FULL / jnp.exp2(code * (1.0 / STEPS))
        quanta.append(jnp.round(piece * unit))
        codes.append(code)
    lane = lax.broadcasted_iota(jnp.int32, (one.shape[0], LANES), 1)
    quanta.append(jnp.where(lane < HALF, codes[0], codes[1]))
    return [q.astype(jnp.int32).astype(I16) for q in quanta]


def decode(packed, first, width):
    code = packed[:, width:].astype(jnp.int32).astype(F32)
    out = []
    for lane, low, high in ((0, 0, first), (HALF, first, width)):
        unit = jnp.exp2(code[:, lane : lane + 1] * (1.0 / STEPS)) * (1.0 / FULL)
        out.append(packed[:, low:high].astype(jnp.int32).astype(F32) * unit)
    return out


def put_encoded(ref, one, two):
    first, width = one.shape[1], one.shape[1] + two.shape[1]
    ref[:, :first], ref[:, first:width], ref[:, width:] = encode(one, two)


def gradients(step, scale, offsets, codes, block, grad, w_second, hidden, twice, dcodes, dpre):
    def put(at, value):
        small = (scale * (grad[at, :] - value)).astype(BF16)
        dcodes[at, :] = small
        wide = dot_nt(small, w_second[...])
        dpre[at, :] = jnp.where(hidden[at, :] > 0, wide, 0.0).astype(BF16)

    repulsion(codes, block, offsets[step], twice, put)


def last_body(step, scale, offsets, bit, codes, block, grad, w_second, hidden, inputs_t, hidden_t, keep, send, *scratch):
    gradients(step, scale, offsets, codes, block, grad, w_second, hidden, *scratch)
    dcodes, dpre = scratch[1:]
    first = dpre.shape[1]
    rows = keep.shape[1]
    mine = bit[0]
    for a in range(keep.shape[0]):
        rows_of = pl.ds(pl.multiple_of((2 * a + 1 - mine) * rows, rows), rows)
        one, two = dot(inputs_t[rows_of, :], dpre[...]), dot(hidden_t[rows_of, :], dcodes[...])
        put_encoded(send.at[a], one, two)
    for a in range(keep.shape[0]):
        rows_of = pl.ds(pl.multiple_of((2 * a + mine) * rows, rows), rows)
        keep[a, :, :first] = dot(inputs_t[rows_of, :], dpre[...])
        keep[a, :, first:] = dot(hidden_t[rows_of, :], dcodes[...])


def last_plain_body(step, scale, offsets, codes, block, grad, w_second, hidden, inputs_t, hidden_t, one, two, *scratch):
    gradients(step, scale, offsets, codes, block, grad, w_second, hidden, *scratch)
    dcodes, dpre = scratch[1:]
    one[...] = dot(inputs_t[...], dpre[...])
    two[...] = dot(hidden_t[...], dcodes[...])


def summed(held, got, first):
    one, two = decode(got, first, held.shape[-1])
    return held[:, :first] + one, held[:, first:] + two


def stage_body(first, bit, held, got, keep, send):
    mine = bit[0]
    for a in range(held.shape[0]):
        put_encoded(send.at[a], *summed(held.at[a, 1 - mine], got.at[a, 1 - mine], first))
    for a in range(held.shape[0]):
        keep[a, :, :first], keep[a, :, first:] = summed(held.at[a, mine], got.at[a, mine], first)


def deal_body(first, me, held, got, keep, *sends):
    for k in range(1, held.shape[0]):
        put_encoded(sends[k - 1], *summed(held.at[me[0] ^ k], got.at[me[0] ^ k], first))
    keep[:, :first], keep[:, first:] = summed(held.at[me[0]], got.at[me[0]], first)


def close_body(first, held, *refs):
    one, two = held[:, :first], held[:, first:]
    for got in refs[:-1]:
        more = decode(got, first, held.shape[1])
        one, two = one + more[0], two + more[1]
    put_encoded(refs[-1], one, two)


def spread_body(first, me, *refs):
    one, two = refs[-2:]
    width = first + two.shape[1]
    for place, ref in enumerate(refs[:-2]):
        rows = ref.shape[0]
        at = pl.ds(pl.multiple_of((me[0] ^ place) * rows, rows), rows)
        one[at, :], two[at, :] = decode(ref, first, width)


def from_behind(block, axis, distance):
    devices = range(lax.axis_size(axis))
    route = [((i - distance) % len(devices), i) for i in devices]
    return lax.ppermute(block, axis, route)


def swapped(block, axis, bit):
    return lax.ppermute(block, axis, [(i, i ^ bit) for i in range(lax.axis_size(axis))])


def bits(count):
    return [1 << b for b in range(count.bit_length() - 1)]


def shards(inputs, w_first, w_second, requests, slots, counts, edge_weight, offsets):
    rows = inputs.shape[0]
    width = w_second.shape[1]
    peers = lax.axis_size("wide")
    group = lax.axis_size("narrow")
    din, hid = w_first.shape
    total_rows = rows * peers * group
    powers = peers & (peers - 1) == 0 and group & (group - 1) == 0 and peers > 1 and group > 1
    assert powers, "axis sizes"
    wide, narrow = lax.axis_index("wide"), lax.axis_index("narrow")
    w_id, n_id = (index.reshape(1).astype(jnp.int32) for index in (wide, narrow))
    pre = jnp.dot(inputs, w_first, preferred_element_type=F32)
    hidden = jnp.maximum(pre, 0.0).astype(BF16)
    codes = jnp.dot(hidden, w_second, preferred_element_type=F32)
    sent = codes.astype(BF16)
    steps = offsets.shape[0]
    blocks = []
    for step in range(steps):
        blocks.append(from_behind(sent if step < 2 else blocks[step - 2], "narrow", min(step, 1) + 1))
    near = [sent[None]]
    for bit in bits(peers):
        moved = near[0] if bit == 1 else jnp.concatenate(near)
        near.append(swapped(moved, "wide", bit))
    inputs_t, hidden_t = call(
        flip_body,
        (jax.ShapeDtypeStruct((din, rows), BF16), jax.ShapeDtypeStruct((hid, rows), BF16)),
        0,
        2,
    )(inputs, hidden)
    like = jax.ShapeDtypeStruct(codes.shape, F32)
    twice = twice_of(rows, width)

    def far(step, grad):
        given = () if grad is None else (grad,)
        body = functools.partial(far_body, step, bool(given))
        return call(body, like, 1, 2 + len(given), [twice])(offsets, codes, blocks[step], *given)

    grad = None
    early = max(steps - 2, 1)
    for step in range(early):
        grad = far(step, grad)
    table = pltpu.VMEM((peers * requests.shape[1], width), BF16)
    grad = call(near_body, like, 1, 6 + len(near), [table])(
        w_id, codes, requests, slots, counts[:, None], edge_weight, grad, *near
    )
    for step in range(early, steps - 1):
        grad = far(step, grad)
    scale = 2.0 / (slots.shape[1] * math.sqrt(total_rows))
    chunk = din // (peers * group)
    scratch = [twice, pltpu.VMEM((rows, width), BF16), pltpu.VMEM((rows, hid), BF16)]
    if din != hid or chunk % 16 or din % (peers * group):
        one, two = call(
            functools.partial(last_plain_body, steps - 1, scale),
            (jax.ShapeDtypeStruct((din, hid), F32), jax.ShapeDtypeStruct((hid, width), F32)),
            1,
            7,
            scratch,
        )(offsets, codes, blocks[-1], grad, w_second, hidden, inputs_t, hidden_t)
        owned = (
            lax.psum_scatter(one, "wide", scatter_dimension=0, tiled=True),
            lax.psum_scatter(two, "wide", scatter_dimension=0, tiled=True),
        )
        return lax.psum(owned, "narrow")

    first, full = hid, hid + width

    def plain(*shape):
        return jax.ShapeDtypeStruct((*shape, full), F32)

    def coded(*shape):
        return jax.ShapeDtypeStruct((*shape, full + LANES), I16)

    plan = [(bit, peers // (2 * bit), din // peers) for bit in bits(peers)]
    keep = got = None
    for bit, groups, lines in plan:
        side = (w_id // bit) % 2
        halves = (plain(groups, lines), coded(groups, lines))
        if keep is None:
            body = functools.partial(last_body, steps - 1, scale)
            keep, send = call(body, halves, 2, 7, scratch)(
                offsets, side, codes, blocks[-1], grad, w_second, hidden, inputs_t, hidden_t
            )
        else:
            keep, send = call(functools.partial(stage_body, first), halves, 1, 2)(
                side, keep.reshape(groups, 2, lines, full), got.reshape(groups, 2, lines, full + LANES)
            )
        got = swapped(send, "wide", bit)
    keep, *sends = call(
        functools.partial(deal_body, first), (plain(chunk),) + (coded(chunk),) * (group - 1), 1, 2
    )(n_id, keep.reshape(group, chunk, full), got.reshape(group, chunk, full + LANES))
    gots = [swapped(send, "narrow", k + 1) for k, send in enumerate(sends)]
    mine = call(functools.partial(close_body, first), coded(chunk), 0, group)(keep, *gots)
    pieces = [mine] + [swapped(mine, "narrow", k) for k in range(1, group)]
    return call(
        functools.partial(spread_body, first),
        (
            jax.ShapeDtypeStruct((din // peers, hid), F32),
            jax.ShapeDtypeStruct((hid // peers, width), F32),
        ),
        1,
        group,
    )(n_id, *pieces)


def solution(mesh):
    return jax.shard_map(
        shards,
        mesh=mesh,
        in_specs=(
            P(("wide", "narrow"), None),
            P(),
            P(),
            P(("wide", "narrow"), None),
            P(("wide", "narrow"), None),
            P(("wide", "narrow")),
            P(("wide", "narrow"), None),
            P(),
        ),
        out_specs=(P("wide", None), P("wide", None)),
        check_vma=False,
    )
```

```python
import functools
import math

import jax
import jax.numpy as jnp
from jax import lax
from jax.experimental import pallas as pl
from jax.experimental.pallas import tpu as pltpu
from jax.sharding import PartitionSpec as P


NEGW = 8
TILE = 128
PACK = 16
LANES = 128
HALF = LANES // 2
FULL = 32000.0
STEPS = 128.0
TINY = 1e-30

F32 = jnp.float32
BF16 = jnp.bfloat16
I16 = jnp.int16
VMEM = pl.BlockSpec(memory_space=pltpu.VMEM)
SMEM = pl.BlockSpec(memory_space=pltpu.SMEM)


def call(body, out_shape, n_scalars, n_arrays, scratch=(), mib=16):
    many = isinstance(out_shape, (list, tuple))
    return pl.pallas_call(
        body,
        out_shape=out_shape,
        in_specs=[SMEM] * n_scalars + [VMEM] * n_arrays,
        out_specs=[VMEM] * len(out_shape) if many else VMEM,
        scratch_shapes=list(scratch),
        compiler_params=pltpu.CompilerParams(vmem_limit_bytes=mib * 1024 * 1024),
    )


def dot(a, b):
    return lax.dot_general(a, b, (((1,), (0,)), ((), ())), preferred_element_type=F32)


def dot_nt(a, b):
    return lax.dot_general(a, b, (((1,), (1,)), ((), ())), preferred_element_type=F32)


def parts(value, count):
    out = []
    for _ in range(count):
        part = value.astype(BF16)
        out.append(part)
        value = value - part.astype(F32)
    return out


def distances(y, z):
    rows = y.shape[0]
    gram = dot_nt(jnp.concatenate(parts(y, 3), axis=0), z)
    gram = gram[:rows] + gram[rows : 2 * rows] + gram[2 * rows :]
    zf = z.astype(F32)
    z_norm = jnp.broadcast_to(jnp.sum(zf * zf, axis=1, keepdims=True), (z.shape[0], rows)).T
    y_norm = jnp.sum(y * y, axis=1, keepdims=True)
    return jnp.maximum(y_norm + z_norm - 2.0 * gram, 0.0) * (1.0 / z.shape[1])


def pull(y, z, coef):
    rows = y.shape[0]
    high, low = parts(coef, 2)
    total = jnp.sum(high.astype(F32) + low.astype(F32), axis=1, keepdims=True)
    mixed = dot(jnp.concatenate([high, low], axis=0), z)
    return y * total - (mixed[:rows] + mixed[rows:])


def forward_body(inputs, w_first, w_second, hidden, codes, sent):
    tile = min(inputs.shape[0], 2 * TILE)
    for at in range(0, inputs.shape[0], tile):
        rows_of = slice(at, at + tile)
        hidden[rows_of, :] = jnp.maximum(dot(inputs[rows_of, :], w_first[...]), 0.0).astype(BF16)
        value = dot(hidden[rows_of, :], w_second[...])
        codes[rows_of, :] = value
        sent[rows_of, :] = value.astype(BF16)


def flip_body(inputs, hidden, inputs_t, hidden_t):
    inputs_t[...] = inputs[...].T
    hidden_t[...] = hidden[...].T


def weight_body(slots, counts, edges, out, total):
    tile = 32
    rows = slots.shape[1]
    for at in range(0, out.shape[1], tile):
        place = at + lax.broadcasted_iota(jnp.int32, (tile, rows), 0)
        weight = jnp.zeros((tile, rows), F32)
        for k in range(slots.shape[0]):
            live = jnp.where(k < counts[...], edges[k : k + 1, :].astype(F32), 0.0)
            weight = weight + jnp.where(place == slots[k : k + 1, :], live, 0.0)
        total[at : at + tile, :] = weight.astype(BF16)
    out[...] = total[...].T


def near_body(me, codes, requests, weight, grad, *rest):
    out, table = rest[-2:]
    cap = requests.shape[1]
    for place, block in enumerate(rest[:-2]):
        asked = requests[pl.ds(me[0] ^ place, 1), :]
        hot = lax.broadcasted_iota(jnp.int32, (block.shape[0], cap), 0) == asked
        hot = jnp.where(hot, 1.0, 0.0).astype(BF16).T
        at = pl.ds(pl.multiple_of((me[0] ^ place) * cap, cap), cap)
        table[at, :] = dot(hot, block[...]).astype(BF16)
    tile = min(codes.shape[0], TILE)
    part = 2 * tile
    for at in range(0, codes.shape[0], tile):
        rows_of = slice(at, at + tile)
        y = codes[rows_of, :]
        total = grad[rows_of, :]
        for low in range(0, table.shape[0], part):
            z = table[low : low + part, :]
            strength = weight[rows_of, low : low + part].astype(F32)
            total = total + pull(y, z, strength / (1.0 + distances(y, z)))
        out[rows_of, :] = total


def repulsion(codes, block, offset, twice, put):
    rows = block.shape[0]
    tile = min(rows, TILE)
    window = tile + max(tile, LANES)
    for at in range(0, twice.shape[0], rows):
        end = min(rows, twice.shape[0] - at)
        twice[at : at + end, :] = block[:end, :]
    start = (offset // PACK) * PACK
    shape = (tile, window)
    place = lax.broadcasted_iota(jnp.int32, shape, 1) - lax.broadcasted_iota(jnp.int32, shape, 0)
    place = place - (offset - start)
    band = (place >= 0) & (place < NEGW)
    for at in range(0, rows, tile):
        y = codes[at : at + tile, :]
        z = twice[pl.ds(pl.multiple_of(start + at, PACK), window), :]
        dist = distances(y, z)
        onep = 1.0 + dist
        coef = jnp.where(band, 1.0 / (onep * (dist + 0.1 * onep)), 0.0)
        put(slice(at, at + tile), pull(y, z, coef))


def twice_of(rows, width):
    tile = min(rows, TILE)
    return pltpu.VMEM((2 * rows + max(tile, LANES), width), BF16)


def far_body(step, started, offsets, codes, block, *rest):
    grad, out, twice = rest if started else (None,) + rest

    def put(at, value):
        out[at, :] = grad[at, :] - value if started else -value

    repulsion(codes, block, offsets[step], twice, put)


def encode(one, two):
    quanta, codes = [], []
    for piece in (one, two):
        top = jnp.maximum(jnp.max(jnp.abs(piece), axis=1, keepdims=True), TINY)
        code = jnp.ceil(jnp.log2(top) * STEPS)
        unit = FULL * jnp.exp2(code * (-1.0 / STEPS))
        quanta.append(jnp.round(piece * unit))
        codes.append(code)
    lane = lax.broadcasted_iota(jnp.int32, (one.shape[0], LANES), 1)
    quanta.append(jnp.where(lane < HALF, codes[0], codes[1]))
    return [q.astype(jnp.int32).astype(I16) for q in quanta]


def decode(packed, first, width):
    code = packed[:, width:].astype(jnp.int32).astype(F32)
    out = []
    for lane, low, high in ((0, 0, first), (HALF, first, width)):
        unit = jnp.exp2(code[:, lane : lane + 1] * (1.0 / STEPS)) * (1.0 / FULL)
        out.append(packed[:, low:high].astype(jnp.int32).astype(F32) * unit)
    return out


def put_encoded(ref, one, two):
    first, width = one.shape[1], one.shape[1] + two.shape[1]
    ref[:, :first], ref[:, first:width], ref[:, width:] = encode(one, two)


def gradients(step, scale, offsets, codes, block, grad, w_second, hidden, twice, dcodes, dpre):
    def put(at, value):
        small = (scale * (grad[at, :] - value)).astype(BF16)
        dcodes[at, :] = small
        wide = dot_nt(small, w_second[...])
        dpre[at, :] = jnp.where(hidden[at, :] > 0, wide, 0.0).astype(BF16)

    repulsion(codes, block, offsets[step], twice, put)


def last_body(step, scale, offsets, bit, codes, block, grad, w_second, hidden, inputs_t, hidden_t, keep, send, *scratch):
    gradients(step, scale, offsets, codes, block, grad, w_second, hidden, *scratch)
    dcodes, dpre = scratch[1:]
    first = dpre.shape[1]
    rows = keep.shape[1]
    mine = bit[0]
    for a in range(keep.shape[0]):
        rows_of = pl.ds(pl.multiple_of((2 * a + 1 - mine) * rows, rows), rows)
        one, two = dot(inputs_t[rows_of, :], dpre[...]), dot(hidden_t[rows_of, :], dcodes[...])
        put_encoded(send.at[a], one, two)
    for a in range(keep.shape[0]):
        rows_of = pl.ds(pl.multiple_of((2 * a + mine) * rows, rows), rows)
        keep[a, :, :first] = dot(inputs_t[rows_of, :], dpre[...])
        keep[a, :, first:] = dot(hidden_t[rows_of, :], dcodes[...])


def last_plain_body(step, scale, offsets, codes, block, grad, w_second, hidden, inputs_t, hidden_t, one, two, *scratch):
    gradients(step, scale, offsets, codes, block, grad, w_second, hidden, *scratch)
    dcodes, dpre = scratch[1:]
    one[...] = dot(inputs_t[...], dpre[...])
    two[...] = dot(hidden_t[...], dcodes[...])


def summed(held, got, first):
    one, two = decode(got, first, held.shape[-1])
    return held[:, :first] + one, held[:, first:] + two


def stage_body(first, bit, held, got, keep, send):
    mine = bit[0]
    for a in range(held.shape[0]):
        put_encoded(send.at[a], *summed(held.at[a, 1 - mine], got.at[a, 1 - mine], first))
    for a in range(held.shape[0]):
        keep[a, :, :first], keep[a, :, first:] = summed(held.at[a, mine], got.at[a, mine], first)


def deal_body(first, me, held, got, keep, *sends):
    for k in range(1, held.shape[0]):
        put_encoded(sends[k - 1], *summed(held.at[me[0] ^ k], got.at[me[0] ^ k], first))
    keep[:, :first], keep[:, first:] = summed(held.at[me[0]], got.at[me[0]], first)


def close_body(first, held, *refs):
    one, two = held[:, :first], held[:, first:]
    for got in refs[:-1]:
        more = decode(got, first, held.shape[1])
        one, two = one + more[0], two + more[1]
    put_encoded(refs[-1], one, two)


def spread_body(first, me, *refs):
    one, two = refs[-2:]
    width = first + two.shape[1]
    for place, ref in enumerate(refs[:-2]):
        rows = ref.shape[0]
        at = pl.ds(pl.multiple_of((me[0] ^ place) * rows, rows), rows)
        one[at, :], two[at, :] = decode(ref, first, width)


def from_behind(block, axis, distance):
    devices = range(lax.axis_size(axis))
    route = [((i - distance) % len(devices), i) for i in devices]
    return lax.ppermute(block, axis, route)


def swapped(block, axis, bit):
    return lax.ppermute(block, axis, [(i, i ^ bit) for i in range(lax.axis_size(axis))])


def bits(count):
    return [1 << b for b in range(count.bit_length() - 1)]


def shards(inputs, w_first, w_second, requests, slots, counts, edge_weight, offsets):
    rows = inputs.shape[0]
    width = w_second.shape[1]
    peers = lax.axis_size("wide")
    group = lax.axis_size("narrow")
    din, hid = w_first.shape
    total_rows = rows * peers * group
    powers = peers & (peers - 1) == 0 and group & (group - 1) == 0 and peers > 1 and group > 1
    assert powers, "axis sizes"
    wide, narrow = lax.axis_index("wide"), lax.axis_index("narrow")
    w_id, n_id = (index.reshape(1).astype(jnp.int32) for index in (wide, narrow))
    hidden, codes, sent = call(
        forward_body,
        (
            jax.ShapeDtypeStruct((rows, hid), BF16),
            jax.ShapeDtypeStruct((rows, width), F32),
            jax.ShapeDtypeStruct((rows, width), BF16),
        ),
        0,
        3,
    )(inputs, w_first, w_second)
    steps = offsets.shape[0]
    blocks = []
    for step in range(steps):
        source = sent if step < 2 else blocks[step - 2]
        blocks.append(from_behind(source, "narrow", min(step, 1) + 1))
    near = [sent]
    for bit in bits(peers):
        near += [swapped(block, "wide", bit) for block in near]
    inputs_t, hidden_t = call(
        flip_body,
        (jax.ShapeDtypeStruct((din, rows), BF16), jax.ShapeDtypeStruct((hid, rows), BF16)),
        0,
        2,
    )(inputs, hidden)
    size = peers * requests.shape[1]
    weight = call(
        weight_body,
        jax.ShapeDtypeStruct((rows, size), BF16),
        0,
        3,
        [pltpu.VMEM((size, rows), BF16)],
    )(slots.T, counts[None], edge_weight.T)
    like = jax.ShapeDtypeStruct(codes.shape, F32)
    twice = twice_of(rows, width)

    def far(step, grad):
        given = () if grad is None else (grad,)
        body = functools.partial(far_body, step, bool(given))
        return call(body, like, 1, 2 + len(given), [twice])(offsets, codes, blocks[step], *given)

    grad = None
    early = max(steps - 2, 1)
    for step in range(early):
        grad = far(step, grad)
    grad = call(near_body, like, 1, 4 + len(near), [pltpu.VMEM((size, width), BF16)])(
        w_id, codes, requests, weight, grad, *near
    )
    for step in range(early, steps - 1):
        grad = far(step, grad)
    scale = 2.0 / (slots.shape[1] * math.sqrt(total_rows))
    chunk = din // (peers * group)
    scratch = [twice, pltpu.VMEM((rows, width), BF16), pltpu.VMEM((rows, hid), BF16)]
    if din != hid or chunk % 16 or din % (peers * group):
        one, two = call(
            functools.partial(last_plain_body, steps - 1, scale),
            (jax.ShapeDtypeStruct((din, hid), F32), jax.ShapeDtypeStruct((hid, width), F32)),
            1,
            7,
            scratch,
        )(offsets, codes, blocks[-1], grad, w_second, hidden, inputs_t, hidden_t)
        owned = (
            lax.psum_scatter(one, "wide", scatter_dimension=0, tiled=True),
            lax.psum_scatter(two, "wide", scatter_dimension=0, tiled=True),
        )
        return lax.psum(owned, "narrow")

    first, full = hid, hid + width

    def plain(*shape):
        return jax.ShapeDtypeStruct((*shape, full), F32)

    def coded(*shape):
        return jax.ShapeDtypeStruct((*shape, full + LANES), I16)

    plan = [(bit, peers // (2 * bit), din // peers) for bit in bits(peers)]
    keep = got = None
    for bit, groups, lines in plan:
        side = (w_id // bit) % 2
        halves = (plain(groups, lines), coded(groups, lines))
        if keep is None:
            body = functools.partial(last_body, steps - 1, scale)
            keep, send = call(body, halves, 2, 7, scratch)(
                offsets, side, codes, blocks[-1], grad, w_second, hidden, inputs_t, hidden_t
            )
        else:
            keep, send = call(functools.partial(stage_body, first), halves, 1, 2)(
                side, keep.reshape(groups, 2, lines, full), got.reshape(groups, 2, lines, full + LANES)
            )
        got = swapped(send, "wide", bit)
    keep, *sends = call(
        functools.partial(deal_body, first), (plain(chunk),) + (coded(chunk),) * (group - 1), 1, 2
    )(n_id, keep.reshape(group, chunk, full), got.reshape(group, chunk, full + LANES))
    gots = [swapped(send, "narrow", k + 1) for k, send in enumerate(sends)]
    mine = call(functools.partial(close_body, first), coded(chunk), 0, group)(keep, *gots)
    pieces = [mine] + [swapped(mine, "narrow", k) for k in range(1, group)]
    return call(
        functools.partial(spread_body, first),
        (
            jax.ShapeDtypeStruct((din // peers, hid), F32),
            jax.ShapeDtypeStruct((hid // peers, width), F32),
        ),
        1,
        group,
    )(n_id, *pieces)


def solution(mesh):
    return jax.shard_map(
        shards,
        mesh=mesh,
        in_specs=(
            P(("wide", "narrow"), None),
            P(),
            P(),
            P(("wide", "narrow"), None),
            P(("wide", "narrow"), None),
            P(("wide", "narrow")),
            P(("wide", "narrow"), None),
            P(),
        ),
        out_specs=(P("wide", None), P("wide", None)),
        check_vma=False,
    )
```

```python
import functools
import math

import jax
import jax.numpy as jnp
from jax import lax
from jax.experimental import pallas as pl
from jax.experimental.pallas import tpu as pltpu
from jax.sharding import PartitionSpec as P


NEGW = 8
TILE = 128
PACK = 16
LANES = 128
HALF = LANES // 2
FULL = 32000.0
STEPS = 128.0
TINY = 1e-30

F32 = jnp.float32
BF16 = jnp.bfloat16
I16 = jnp.int16
VMEM = pl.BlockSpec(memory_space=pltpu.VMEM)
SMEM = pl.BlockSpec(memory_space=pltpu.SMEM)


def digit(me, below, count):
    return lax.rem(lax.div(me[0], below), count)


def call(body, out_shape, n_scalars, n_arrays, scratch=(), mib=16):
    many = isinstance(out_shape, (list, tuple))
    return pl.pallas_call(
        body,
        out_shape=out_shape,
        in_specs=[SMEM] * n_scalars + [VMEM] * n_arrays,
        out_specs=[VMEM] * len(out_shape) if many else VMEM,
        scratch_shapes=list(scratch),
        compiler_params=pltpu.CompilerParams(vmem_limit_bytes=mib * 1024 * 1024),
    )


def dot(a, b):
    return lax.dot_general(a, b, (((1,), (0,)), ((), ())), preferred_element_type=F32)


def dot_nt(a, b):
    return lax.dot_general(a, b, (((1,), (1,)), ((), ())), preferred_element_type=F32)


def parts(value, count):
    out = []
    for _ in range(count):
        part = value.astype(BF16)
        out.append(part)
        value = value - part.astype(F32)
    return out


def distances(y, z):
    rows = y.shape[0]
    gram = dot_nt(jnp.concatenate(parts(y, 3), axis=0), z)
    gram = gram[:rows] + gram[rows : 2 * rows] + gram[2 * rows :]
    zf = z.astype(F32)
    z_norm = jnp.broadcast_to(jnp.sum(zf * zf, axis=1, keepdims=True), (z.shape[0], rows)).T
    y_norm = jnp.sum(y * y, axis=1, keepdims=True)
    return jnp.maximum(y_norm + z_norm - 2.0 * gram, 0.0) * (1.0 / z.shape[1])


def pull(y, z, coef):
    rows = y.shape[0]
    high, low = parts(coef, 2)
    total = jnp.sum(high.astype(F32) + low.astype(F32), axis=1, keepdims=True)
    mixed = dot(jnp.concatenate([high, low], axis=0), z)
    return y * total - (mixed[:rows] + mixed[rows:])


def forward_body(me, inputs, w_first, w_second, hidden, codes, sent, block, first, second, sems):
    del me
    count = first.shape[0]
    size = first.shape[2]
    copies = [pltpu.make_async_copy(inputs, block, sems.at[0])]
    for c in range(count):
        columns = w_first.at[:, c * size : (c + 1) * size]
        copies.append(pltpu.make_async_copy(columns, first.at[c], sems.at[c + 1]))
    copies.append(pltpu.make_async_copy(w_second, second, sems.at[count + 1]))
    for copy in copies:
        copy.start()
    copies[0].wait()
    for c in range(count):
        copies[c + 1].wait()
        columns = slice(c * size, (c + 1) * size)
        hidden[:, columns] = jnp.maximum(dot(block[...], first[c]), 0.0).astype(BF16)
    copies[-1].wait()
    value = dot(hidden[...], second[...])
    codes[...] = value
    sent[...] = value.astype(BF16)


def flip_body(inputs, hidden, inputs_t, hidden_t):
    inputs_t[...] = inputs[...].T
    hidden_t[...] = hidden[...].T


def weight_body(slots, counts, edges, out, total):
    tile = 32
    rows = slots.shape[1]
    for at in range(0, out.shape[1], tile):
        place = at + lax.broadcasted_iota(jnp.int32, (tile, rows), 0)
        weight = jnp.zeros((tile, rows), F32)
        for k in range(slots.shape[0]):
            live = jnp.where(k < counts[...], edges[k : k + 1, :].astype(F32), 0.0)
            weight = weight + jnp.where(place == slots[k : k + 1, :], live, 0.0)
        total[at : at + tile, :] = weight.astype(BF16)
    out[...] = total[...].T


def near_body(group, me, codes, requests, weight, grad, *rest):
    out, table = rest[-2:]
    cap = requests.shape[1]
    wide = digit(me, group, len(rest[:-2]))
    for place, block in enumerate(rest[:-2]):
        asked = requests[pl.ds(wide ^ place, 1), :]
        hot = lax.broadcasted_iota(jnp.int32, (block.shape[0], cap), 0) == asked
        hot = jnp.where(hot, 1.0, 0.0).astype(BF16).T
        at = pl.ds(pl.multiple_of((wide ^ place) * cap, cap), cap)
        table[at, :] = dot(hot, block[...]).astype(BF16)
    tile = min(codes.shape[0], TILE)
    part = 2 * tile
    for at in range(0, codes.shape[0], tile):
        rows_of = slice(at, at + tile)
        y = codes[rows_of, :]
        total = grad[rows_of, :]
        for low in range(0, table.shape[0], part):
            z = table[low : low + part, :]
            strength = weight[rows_of, low : low + part].astype(F32)
            total = total + pull(y, z, strength / (1.0 + distances(y, z)))
        out[rows_of, :] = total


def repulsion(codes, block, offset, twice, put):
    rows = block.shape[0]
    tile = min(rows, TILE)
    window = tile + max(tile, LANES)
    for at in range(0, twice.shape[0], rows):
        end = min(rows, twice.shape[0] - at)
        twice[at : at + end, :] = block[:end, :]
    start = (offset // PACK) * PACK
    shape = (tile, window)
    place = lax.broadcasted_iota(jnp.int32, shape, 1) - lax.broadcasted_iota(jnp.int32, shape, 0)
    place = place - (offset - start)
    band = (place >= 0) & (place < NEGW)
    for at in range(0, rows, tile):
        y = codes[at : at + tile, :]
        z = twice[pl.ds(pl.multiple_of(start + at, PACK), window), :]
        dist = distances(y, z)
        onep = 1.0 + dist
        coef = jnp.where(band, 1.0 / (onep * (dist + 0.1 * onep)), 0.0)
        put(slice(at, at + tile), pull(y, z, coef))


def twice_of(rows, width):
    tile = min(rows, TILE)
    return pltpu.VMEM((2 * rows + max(tile, LANES), width), BF16)


def far_body(step, started, offsets, codes, block, *rest):
    grad, out, twice = rest if started else (None,) + rest

    def put(at, value):
        out[at, :] = grad[at, :] - value if started else -value

    repulsion(codes, block, offsets[step], twice, put)


def encode(one, two):
    quanta, codes = [], []
    for piece in (one, two):
        top = jnp.maximum(jnp.max(jnp.abs(piece), axis=1, keepdims=True), TINY)
        code = jnp.ceil(jnp.log2(top) * STEPS)
        unit = FULL * jnp.exp2(code * (-1.0 / STEPS))
        quanta.append(jnp.round(piece * unit))
        codes.append(code)
    lane = lax.broadcasted_iota(jnp.int32, (one.shape[0], LANES), 1)
    quanta.append(jnp.where(lane < HALF, codes[0], codes[1]))
    return [q.astype(jnp.int32).astype(I16) for q in quanta]


def decode(packed, first, width):
    code = packed[:, width:].astype(jnp.int32).astype(F32)
    out = []
    for lane, low, high in ((0, 0, first), (HALF, first, width)):
        unit = jnp.exp2(code[:, lane : lane + 1] * (1.0 / STEPS)) * (1.0 / FULL)
        out.append(packed[:, low:high].astype(jnp.int32).astype(F32) * unit)
    return out


def put_encoded(ref, one, two):
    first, width = one.shape[1], one.shape[1] + two.shape[1]
    ref[:, :first], ref[:, first:width], ref[:, width:] = encode(one, two)


def gradients(step, scale, offsets, codes, block, grad, w_second, hidden, twice, dcodes, dpre):
    def put(at, value):
        dcodes[at, :] = (scale * (grad[at, :] - value)).astype(BF16)

    repulsion(codes, block, offsets[step], twice, put)
    size = 2 * LANES
    for at in range(0, hidden.shape[1], size):
        columns = slice(at, at + size)
        wide = dot_nt(dcodes[...], w_second[columns, :])
        dpre[:, columns] = jnp.where(hidden[:, columns] > 0, wide, 0.0).astype(BF16)


def give_body(step, scale, below, offsets, me, codes, block, grad, w_second, hidden, inputs_t, hidden_t, send, dcodes, dpre, twice):
    gradients(step, scale, offsets, codes, block, grad, w_second, hidden, twice, dcodes, dpre)
    groups, rows = send.shape[:2]
    one, two = halves(1 - digit(me, below, 2), groups, rows, dcodes, dpre, inputs_t, hidden_t)
    for a in range(groups):
        at = slice(a * rows, (a + 1) * rows)
        put_encoded(send.at[a], one[at], two[at])


def hold_body(below, me, dcodes, dpre, inputs_t, hidden_t, keep):
    groups, rows = keep.shape[:2]
    first = dpre.shape[1]
    one, two = halves(digit(me, below, 2), groups, rows, dcodes, dpre, inputs_t, hidden_t)
    for a in range(groups):
        at = slice(a * rows, (a + 1) * rows)
        keep[a, :, :first], keep[a, :, first:] = one[at], two[at]


def halves(side, groups, rows, dcodes, dpre, inputs_t, hidden_t):
    def taken(ref):
        at = [pl.ds(pl.multiple_of((2 * a + side) * rows, rows), rows) for a in range(groups)]
        return jnp.concatenate([ref[rows_of, :] for rows_of in at], axis=0)

    return dot(taken(inputs_t), dpre[...]), dot(taken(hidden_t), dcodes[...])


def last_plain_body(step, scale, offsets, codes, block, grad, w_second, hidden, inputs_t, hidden_t, one, two, *scratch):
    gradients(step, scale, offsets, codes, block, grad, w_second, hidden, *scratch)
    dcodes, dpre = scratch[1:]
    one[...] = dot(inputs_t[...], dpre[...])
    two[...] = dot(hidden_t[...], dcodes[...])


def summed(held, got, first):
    one, two = decode(got, first, held.shape[-1])
    return held[:, :first] + one, held[:, first:] + two


def stage_body(first, below, me, held, got, keep, send):
    mine = digit(me, below, 2)
    for a in range(held.shape[0]):
        put_encoded(send.at[a], *summed(held.at[a, 1 - mine], got.at[a, 1 - mine], first))
    for a in range(held.shape[0]):
        keep[a, :, :first], keep[a, :, first:] = summed(held.at[a, mine], got.at[a, mine], first)


def part_body(first, belows, me, held, got, p_keep, p_send, q_keep, q_send):
    mine, here = (digit(me, below, 2) for below in belows)
    other, there = 1 - mine, 1 - here
    for j in range(held.shape[2]):
        for bit in range(2):
            at = (other, 0, j, bit)
            put_encoded(p_send.at[j, bit], *summed(held.at[at], got.at[at], first))
        for block in range(2):
            at = (block, 1, j, there)
            put_encoded(q_send.at[block, j], *summed(held.at[at], got.at[at], first))
    for j in range(held.shape[2]):
        for bit in range(2):
            at = (mine, 0, j, bit)
            p_keep[j, bit, :, :first], p_keep[j, bit, :, first:] = summed(held.at[at], got.at[at], first)
        for block in range(2):
            at = (block, 1, j, here)
            q_keep[block, j, :, :first], q_keep[block, j, :, first:] = summed(held.at[at], got.at[at], first)


def cross_body(first, belows, me, p_held, q_held, p_got, q_got, p_keep, q_keep, p_send, q_send):
    mine, here = (digit(me, below, 2) for below in belows)
    other, there = 1 - mine, 1 - here
    for j in range(p_send.shape[0]):
        put_encoded(p_send.at[j], *summed(p_held.at[j, there], p_got.at[j, there], first))
        put_encoded(q_send.at[j], *summed(q_held.at[other, j], q_got.at[other, j], first))
    for j in range(p_send.shape[0]):
        p_keep[j, :, :first], p_keep[j, :, first:] = summed(p_held.at[j, here], p_got.at[j, here], first)
        q_keep[j, :, :first], q_keep[j, :, first:] = summed(q_held.at[mine, j], q_got.at[mine, j], first)


def deal_body(first, me, p_held, q_held, p_got, q_got, keep, *sends):
    pairs = ((p_held, p_got), (q_held, q_got))
    mine = digit(me, 2, p_held.shape[0])
    for k in range(1, p_held.shape[0]):
        for half, (held, got) in enumerate(pairs):
            piece = summed(held.at[mine ^ k], got.at[mine ^ k], first)
            put_encoded(sends[k - 1].at[half], *piece)
    for half, (held, got) in enumerate(pairs):
        keep[half, :, :first], keep[half, :, first:] = summed(held.at[mine], got.at[mine], first)


def close_body(first, held, *refs):
    for half in range(held.shape[0]):
        one, two = held[half, :, :first], held[half, :, first:]
        for got in refs[:-1]:
            more = decode(got.at[half], first, held.shape[2])
            one, two = one + more[0], two + more[1]
        put_encoded(refs[-1].at[half], one, two)


def spread_body(first, me, *refs):
    one, two = refs[-2:]
    width = first + two.shape[1]
    narrow = digit(me, 1, len(refs[:-2]))
    for place, ref in enumerate(refs[:-2]):
        rows = ref.shape[1]
        for half in range(ref.shape[0]):
            at = half * (one.shape[0] // 2) + (narrow ^ place) * rows
            at = pl.ds(pl.multiple_of(at, rows), rows)
            one[at, :], two[at, :] = decode(ref.at[half], first, width)


def from_behind(block, axis, distance):
    devices = range(lax.axis_size(axis))
    route = [((i - distance) % len(devices), i) for i in devices]
    return lax.ppermute(block, axis, route)


def swapped(block, axis, bit):
    return lax.ppermute(block, axis, [(i, i ^ bit) for i in range(lax.axis_size(axis))])


def bits(count):
    return [1 << b for b in range(count.bit_length() - 1)]


def shards(inputs, w_first, w_second, requests, slots, counts, edge_weight, offsets):
    rows = inputs.shape[0]
    width = w_second.shape[1]
    peers = lax.axis_size("wide")
    group = lax.axis_size("narrow")
    din, hid = w_first.shape
    total_rows = rows * peers * group
    powers = peers & (peers - 1) == 0 and group & (group - 1) == 0 and peers > 1 and group > 1
    assert powers, "axis sizes"
    me = lax.axis_index(("wide", "narrow")).reshape(1).astype(jnp.int32)
    count = 4 if hid % (4 * LANES) == 0 else 1
    hidden, codes, sent = pl.pallas_call(
        forward_body,
        out_shape=(
            jax.ShapeDtypeStruct((rows, hid), BF16),
            jax.ShapeDtypeStruct((rows, width), F32),
            jax.ShapeDtypeStruct((rows, width), BF16),
        ),
        in_specs=[SMEM] + [pl.BlockSpec(memory_space=pltpu.HBM)] * 3,
        out_specs=[VMEM] * 3,
        scratch_shapes=[
            pltpu.VMEM(inputs.shape, BF16),
            pltpu.VMEM((count, din, hid // count), BF16),
            pltpu.VMEM(w_second.shape, BF16),
            pltpu.SemaphoreType.DMA((count + 2,)),
        ],
        compiler_params=pltpu.CompilerParams(vmem_limit_bytes=16 * 1024 * 1024),
    )(me, *(pltpu.with_memory_space_constraint(a, pltpu.HBM) for a in (inputs, w_first, w_second)))
    steps = offsets.shape[0]
    blocks = []
    for step in range(steps):
        source = sent if step < 2 else blocks[step - 2]
        blocks.append(from_behind(source, "narrow", min(step, 1) + 1))
    near = [sent]
    for bit in bits(peers):
        near += [swapped(block, "wide", bit) for block in near]
    inputs_t, hidden_t = call(
        flip_body,
        (jax.ShapeDtypeStruct((din, rows), BF16), jax.ShapeDtypeStruct((hid, rows), BF16)),
        0,
        2,
    )(inputs, hidden)
    size = peers * requests.shape[1]
    weight = call(
        weight_body,
        jax.ShapeDtypeStruct((rows, size), BF16),
        0,
        3,
        [pltpu.VMEM((size, rows), BF16)],
    )(slots.T, counts[None], edge_weight.T)
    like = jax.ShapeDtypeStruct(codes.shape, F32)
    twice = twice_of(rows, width)

    def far(step, grad):
        given = () if grad is None else (grad,)
        body = functools.partial(far_body, step, bool(given))
        return call(body, like, 1, 2 + len(given), [twice])(offsets, codes, blocks[step], *given)

    grad = None
    early = max(steps - 2, 1)
    for step in range(early):
        grad = far(step, grad)
    grad = call(functools.partial(near_body, group), like, 1, 4 + len(near), [pltpu.VMEM((size, width), BF16)])(
        me, codes, requests, weight, grad, *near
    )
    for step in range(early, steps - 1):
        grad = far(step, grad)
    scale = 2.0 / (slots.shape[1] * math.sqrt(total_rows))
    chunk = din // (peers * group)
    scratch = [twice, pltpu.VMEM((rows, width), BF16), pltpu.VMEM((rows, hid), BF16)]
    if din != hid or chunk % 32 or din % (peers * group) or peers < 4 or group < 4:
        one, two = call(
            functools.partial(last_plain_body, steps - 1, scale),
            (jax.ShapeDtypeStruct((din, hid), F32), jax.ShapeDtypeStruct((hid, width), F32)),
            1,
            7,
            scratch,
        )(offsets, codes, blocks[-1], grad, w_second, hidden, inputs_t, hidden_t)
        owned = (
            lax.psum_scatter(one, "wide", scatter_dimension=0, tiled=True),
            lax.psum_scatter(two, "wide", scatter_dimension=0, tiled=True),
        )
        return lax.psum(owned, "narrow")

    first, full = hid, hid + width

    def plain(*shape):
        return jax.ShapeDtypeStruct((*shape, full), F32)

    def coded(*shape):
        return jax.ShapeDtypeStruct((*shape, full + LANES), I16)

    keep = got = None
    for bit in bits(peers)[:-1]:
        below = bit * group
        groups, lines = peers // (2 * bit), din // peers
        if keep is None:
            send, dcodes, dpre = call(
                functools.partial(give_body, steps - 1, scale, below),
                (
                    coded(groups, lines),
                    jax.ShapeDtypeStruct((rows, width), BF16),
                    jax.ShapeDtypeStruct((rows, hid), BF16),
                ),
                2,
                7,
                [twice],
            )(offsets, me, codes, blocks[-1], grad, w_second, hidden, inputs_t, hidden_t)
            keep = call(functools.partial(hold_body, below), plain(groups, lines), 1, 4)(me, dcodes, dpre, inputs_t, hidden_t)
        else:
            keep, send = call(
                functools.partial(stage_body, first, below), (plain(groups, lines), coded(groups, lines)), 1, 2
            )(me, keep.reshape(groups, 2, lines, full), got.reshape(groups, 2, lines, full + LANES))
        got = swapped(send, "wide", bit)
    last, lines, others = peers // 2, chunk // 2, group // 2
    belows = (last * group, 1)
    p_keep, p_send, q_keep, q_send = call(
        functools.partial(part_body, first, belows),
        (
            plain(others, 2, lines),
            coded(others, 2, lines),
            plain(2, others, lines),
            coded(2, others, lines),
        ),
        1,
        2,
    )(
        me,
        keep.reshape(2, 2, others, 2, lines, full),
        got.reshape(2, 2, others, 2, lines, full + LANES),
    )
    p_got, q_got = swapped(p_send, "wide", last), swapped(q_send, "narrow", 1)
    p_keep, q_keep, p_send, q_send = call(
        functools.partial(cross_body, first, belows),
        (plain(others, lines),) * 2 + (coded(others, lines),) * 2,
        1,
        4,
    )(me, p_keep, q_keep, p_got, q_got)
    p_got, q_got = swapped(p_send, "narrow", 1), swapped(q_send, "wide", last)
    keep, *sends = call(
        functools.partial(deal_body, first),
        (plain(2, lines),) + (coded(2, lines),) * (others - 1),
        1,
        4,
    )(me, p_keep, q_keep, p_got, q_got)
    gots = [swapped(send, "narrow", 2 * (k + 1)) for k, send in enumerate(sends)]
    mine = call(functools.partial(close_body, first), coded(2, lines), 0, others)(keep, *gots)
    pieces = [mine] + [swapped(mine, "narrow", k) for k in range(1, group)]
    return call(
        functools.partial(spread_body, first),
        (
            jax.ShapeDtypeStruct((din // peers, hid), F32),
            jax.ShapeDtypeStruct((hid // peers, width), F32),
        ),
        1,
        group,
    )(me, *pieces)


def solution(mesh):
    return jax.shard_map(
        shards,
        mesh=mesh,
        in_specs=(
            P(("wide", "narrow"), None),
            P(),
            P(),
            P(("wide", "narrow"), None),
            P(("wide", "narrow"), None),
            P(("wide", "narrow")),
            P(("wide", "narrow"), None),
            P(),
        ),
        out_specs=(P("wide", None), P("wide", None)),
        check_vma=False,
    )
```

```python
import functools
import math

import jax
import jax.numpy as jnp
from jax import lax
from jax.experimental import pallas as pl
from jax.experimental.pallas import tpu as pltpu
from jax.sharding import PartitionSpec as P


NEGW = 8
TILE = 128
PACK = 16
SHARE = 16
LANES = 128
HALF = LANES // 2
FULL = 32000.0
STEPS = 128.0
TINY = 1e-30

F32 = jnp.float32
BF16 = jnp.bfloat16
I16 = jnp.int16
VMEM = pl.BlockSpec(memory_space=pltpu.VMEM)
SMEM = pl.BlockSpec(memory_space=pltpu.SMEM)


def digit(me, below, count):
    return lax.rem(lax.div(me[0], below), count)


def call(body, out_shape, n_scalars, n_arrays, scratch=(), mib=16):
    many = isinstance(out_shape, (list, tuple))
    return pl.pallas_call(
        body,
        out_shape=out_shape,
        in_specs=[SMEM] * n_scalars + [VMEM] * n_arrays,
        out_specs=[VMEM] * len(out_shape) if many else VMEM,
        scratch_shapes=list(scratch),
        compiler_params=pltpu.CompilerParams(vmem_limit_bytes=mib * 1024 * 1024),
    )


def dot(a, b):
    return lax.dot_general(a, b, (((1,), (0,)), ((), ())), preferred_element_type=F32)


def dot_nt(a, b):
    return lax.dot_general(a, b, (((1,), (1,)), ((), ())), preferred_element_type=F32)


def parts(value, count):
    out = []
    for _ in range(count):
        part = value.astype(BF16)
        out.append(part)
        value = value - part.astype(F32)
    return out


def distances(y, z):
    rows = y.shape[0]
    gram = dot_nt(jnp.concatenate(parts(y, 3), axis=0), z)
    gram = gram[:rows] + gram[rows : 2 * rows] + gram[2 * rows :]
    zf = z.astype(F32)
    z_norm = jnp.broadcast_to(jnp.sum(zf * zf, axis=1, keepdims=True), (z.shape[0], rows)).T
    y_norm = jnp.sum(y * y, axis=1, keepdims=True)
    return jnp.maximum(y_norm + z_norm - 2.0 * gram, 0.0) * (1.0 / z.shape[1])


def pull(y, z, coef):
    rows = y.shape[0]
    high, low = parts(coef, 2)
    total = jnp.sum(high.astype(F32) + low.astype(F32), axis=1, keepdims=True)
    mixed = dot(jnp.concatenate([high, low], axis=0), z)
    return y * total - (mixed[:rows] + mixed[rows:])


def forward_body(me, inputs, w_first, w_second, hidden, codes, sent, block, first, second, sems):
    del me
    count = first.shape[0]
    size = first.shape[2]
    copies = [pltpu.make_async_copy(inputs, block, sems.at[0])]
    for c in range(count):
        columns = w_first.at[:, c * size : (c + 1) * size]
        copies.append(pltpu.make_async_copy(columns, first.at[c], sems.at[c + 1]))
    copies.append(pltpu.make_async_copy(w_second, second, sems.at[count + 1]))
    for copy in copies:
        copy.start()
    copies[0].wait()
    for c in range(count):
        copies[c + 1].wait()
        columns = slice(c * size, (c + 1) * size)
        hidden[:, columns] = jnp.maximum(dot(block[...], first[c]), 0.0).astype(BF16)
    copies[-1].wait()
    value = dot(hidden[...], second[...])
    codes[...] = value
    sent[...] = value.astype(BF16)


def flip_body(inputs, hidden, inputs_t, hidden_t):
    inputs_t[...] = inputs[...].T
    hidden_t[...] = hidden[...].T


def weight_body(slots, counts, edges, out, total):
    tile = 32
    rows = slots.shape[1]
    for at in range(0, out.shape[1], tile):
        place = at + lax.broadcasted_iota(jnp.int32, (tile, rows), 0)
        weight = jnp.zeros((tile, rows), F32)
        for k in range(slots.shape[0]):
            live = jnp.where(k < counts[...], edges[k : k + 1, :].astype(F32), 0.0)
            weight = weight + jnp.where(place == slots[k : k + 1, :], live, 0.0)
        total[at : at + tile, :] = weight.astype(BF16)
    out[...] = total[...].T


def near_body(group, me, codes, requests, weight, grad, *rest):
    out, table = rest[-2:]
    cap = requests.shape[1]
    wide = digit(me, group, len(rest[:-2]))
    for place, block in enumerate(rest[:-2]):
        asked = requests[pl.ds(wide ^ place, 1), :]
        hot = lax.broadcasted_iota(jnp.int32, (block.shape[0], cap), 0) == asked
        hot = jnp.where(hot, 1.0, 0.0).astype(BF16).T
        at = pl.ds(pl.multiple_of((wide ^ place) * cap, cap), cap)
        table[at, :] = dot(hot, block[...]).astype(BF16)
    tile = min(codes.shape[0], TILE)
    part = 2 * tile
    for at in range(0, codes.shape[0], tile):
        rows_of = slice(at, at + tile)
        y = codes[rows_of, :]
        total = grad[rows_of, :]
        for low in range(0, table.shape[0], part):
            z = table[low : low + part, :]
            strength = weight[rows_of, low : low + part].astype(F32)
            total = total + pull(y, z, strength / (1.0 + distances(y, z)))
        out[rows_of, :] = total


def repulsion(me, codes, choices, offset, twice, put):
    rows = codes.shape[0]
    block = choices[0][...]
    if len(choices) > 1:
        block = jnp.where(digit(me, 1, 2) > 0, choices[1][...], block)
    tile = min(rows, TILE)
    window = tile + max(tile, LANES)
    for at in range(0, twice.shape[0], rows):
        end = min(rows, twice.shape[0] - at)
        twice[at : at + end, :] = block[:end, :]
    start = (offset // PACK) * PACK
    shape = (tile, window)
    place = lax.broadcasted_iota(jnp.int32, shape, 1) - lax.broadcasted_iota(jnp.int32, shape, 0)
    place = place - (offset - start)
    band = (place >= 0) & (place < NEGW)
    for at in range(0, rows, tile):
        y = codes[at : at + tile, :]
        z = twice[pl.ds(pl.multiple_of(start + at, PACK), window), :]
        dist = distances(y, z)
        onep = 1.0 + dist
        coef = jnp.where(band, 1.0 / (onep * (dist + 0.1 * onep)), 0.0)
        put(slice(at, at + tile), pull(y, z, coef))


def twice_of(rows, width):
    tile = min(rows, TILE)
    return pltpu.VMEM((2 * rows + max(tile, LANES), width), BF16)


def far_body(step, count, me, offsets, codes, *rest):
    choices, rest = rest[:count], rest[count:]
    out, twice = rest[-2:]
    grad = rest[0] if len(rest) > 2 else None

    def put(at, value):
        out[at, :] = -value if grad is None else grad[at, :] - value

    repulsion(me, codes, choices, offsets[step], twice, put)


def encode(one, two):
    quanta, codes = [], []
    for piece in (one, two):
        top = jnp.maximum(jnp.max(jnp.abs(piece), axis=1, keepdims=True), TINY)
        code = jnp.ceil(jnp.log2(top) * STEPS)
        quanta.append(short(jnp.round(piece * (FULL * jnp.exp2(code * (-1.0 / STEPS))))))
        codes.append(code)
    return quanta, codes


def short(value):
    return value.astype(jnp.int32).astype(I16)


def unit_of(code):
    return jnp.exp2(code * (1.0 / STEPS)) * (1.0 / FULL)


def pack(ref, pieces):
    rows = ref.shape[1]
    lane = lax.broadcasted_iota(jnp.int32, (rows, LANES), 1)
    header = jnp.zeros((rows, LANES), F32)
    at = 0
    for k, piece in enumerate(pieces):
        quanta, codes = encode(*piece)
        for quantum in quanta:
            for column in range(0, quantum.shape[1], LANES):
                ref[at] = quantum[:, column : column + LANES]
                at += 1
        for j, code in enumerate(codes):
            header = jnp.where(lane >= SHARE * k + SHARE // 2 * j, code, header)
    ref[at] = short(header)


def unpack(ref, k, first, width):
    tiles = width // LANES
    header = ref[ref.shape[0] - 1].astype(jnp.int32).astype(F32)
    out = []
    for j, (low, high) in enumerate(((0, first // LANES), (first // LANES, tiles))):
        lane = SHARE * k + SHARE // 2 * j
        unit = unit_of(header[:, lane : lane + 1])
        value = [ref[k * tiles + g].astype(jnp.int32).astype(F32) for g in range(low, high)]
        out.append(jnp.concatenate(value, axis=1) * unit)
    return out


def decode(packed, first, width):
    code = packed[:, width:].astype(jnp.int32).astype(F32)
    out = []
    for lane, low, high in ((0, 0, first), (HALF, first, width)):
        unit = unit_of(code[:, lane : lane + 1])
        out.append(packed[:, low:high].astype(jnp.int32).astype(F32) * unit)
    return out


def put_encoded(ref, one, two):
    first, width = one.shape[1], one.shape[1] + two.shape[1]
    (ref[:, :first], ref[:, first:width]), codes = encode(one, two)
    lane = lax.broadcasted_iota(jnp.int32, (one.shape[0], LANES), 1)
    ref[:, width:] = short(jnp.where(lane < HALF, codes[0], codes[1]))


def gradients(step, scale, me, offsets, codes, choices, grad, w_second, hidden, twice, dcodes, dpre):
    def put(at, value):
        dcodes[at, :] = (scale * (grad[at, :] - value)).astype(BF16)

    repulsion(me, codes, choices, offsets[step], twice, put)
    size = 2 * LANES
    for at in range(0, hidden.shape[1], size):
        columns = slice(at, at + size)
        wide = dot_nt(dcodes[...], w_second[columns, :])
        dpre[:, columns] = jnp.where(hidden[:, columns] > 0, wide, 0.0).astype(BF16)


def give_body(step, scale, below, me, offsets, codes, *rest):
    *choices, grad, w_second, hidden, inputs_t, hidden_t, send, dcodes, dpre, twice = rest
    gradients(step, scale, me, offsets, codes, choices, grad, w_second, hidden, twice, dcodes, dpre)
    groups, rows = send.shape[:2]
    one, two = halves(1 - digit(me, below, 2), groups, rows, dcodes, dpre, inputs_t, hidden_t)
    for a in range(groups):
        at = slice(a * rows, (a + 1) * rows)
        put_encoded(send.at[a], one[at], two[at])


def hold_body(below, me, dcodes, dpre, inputs_t, hidden_t, keep):
    groups, rows = keep.shape[:2]
    first = dpre.shape[1]
    one, two = halves(digit(me, below, 2), groups, rows, dcodes, dpre, inputs_t, hidden_t)
    for a in range(groups):
        at = slice(a * rows, (a + 1) * rows)
        keep[a, :, :first], keep[a, :, first:] = one[at], two[at]


def halves(side, groups, rows, dcodes, dpre, inputs_t, hidden_t):
    def taken(ref):
        at = [pl.ds(pl.multiple_of((2 * a + side) * rows, rows), rows) for a in range(groups)]
        return jnp.concatenate([ref[rows_of, :] for rows_of in at], axis=0)

    return dot(taken(inputs_t), dpre[...]), dot(taken(hidden_t), dcodes[...])


def last_plain_body(step, scale, me, offsets, codes, *rest):
    *choices, grad, w_second, hidden, inputs_t, hidden_t, one, two, twice, dcodes, dpre = rest
    gradients(step, scale, me, offsets, codes, choices, grad, w_second, hidden, twice, dcodes, dpre)
    one[...] = dot(inputs_t[...], dpre[...])
    two[...] = dot(hidden_t[...], dcodes[...])


def summed(held, got, first):
    one, two = decode(got, first, held.shape[-1])
    return held[:, :first] + one, held[:, first:] + two


def stage_body(first, below, me, held, got, keep, send):
    mine = digit(me, below, 2)
    for a in range(held.shape[0]):
        put_encoded(send.at[a], *summed(held.at[a, 1 - mine], got.at[a, 1 - mine], first))
    for a in range(held.shape[0]):
        keep[a, :, :first], keep[a, :, first:] = summed(held.at[a, mine], got.at[a, mine], first)


def part_index(below, me, others):
    mine, here, place = digit(me, below, 2), digit(me, 1, 2), digit(me, 2, others)

    def p_at(side, k, r):
        return (mine ^ side, 0, place ^ k, here ^ r)

    def q_at(side, r, k):
        return (mine ^ r, 1, place ^ k, here ^ side)

    return p_at, q_at


def part_send_body(first, below, half, me, held, got, send):
    others = held.shape[2]
    index = part_index(below, me, others)[half]
    pairs = [(i, j) for i in range((others, 2)[half]) for j in range((2, others)[half])]
    pack(send, [summed(held.at[index(1, *pair)], got.at[index(1, *pair)], first) for pair in pairs])


def part_keep_body(first, below, me, held, got, p_keep, q_keep):
    others = held.shape[2]
    p_at, q_at = part_index(below, me, others)
    for k in range(others):
        for r in range(2):
            at = p_at(0, k, r)
            p_keep[k, r, :, :first], p_keep[k, r, :, first:] = summed(held.at[at], got.at[at], first)
            at = q_at(0, r, k)
            q_keep[r, k, :, :first], q_keep[r, k, :, first:] = summed(held.at[at], got.at[at], first)


def joined(held, got, k, first):
    one, two = unpack(got, k, first, held.shape[-1])
    return held[:, :first] + one, held[:, first:] + two


def cross_send_body(first, p_held, q_held, p_got, q_got, p_send, q_send):
    others = p_held.shape[0]
    pack(p_send, [joined(p_held.at[k, 1], p_got, 2 * k + 1, first) for k in range(others)])
    pack(q_send, [joined(q_held.at[1, k], q_got, others + k, first) for k in range(others)])


def cross_keep_body(first, p_held, q_held, p_got, q_got, p_keep, q_keep):
    for k in range(p_held.shape[0]):
        p_keep[k, :, :first], p_keep[k, :, first:] = joined(p_held.at[k, 0], p_got, 2 * k, first)
        q_keep[k, :, :first], q_keep[k, :, first:] = joined(q_held.at[0, k], q_got, k, first)


def deal_send_body(first, p_held, q_held, p_got, q_got, *sends):
    pairs = ((p_held, p_got), (q_held, q_got))
    for k, send in enumerate(sends, 1):
        pack(send, [joined(held.at[k], got, k, first) for held, got in pairs])


def deal_keep_body(first, p_held, q_held, p_got, q_got, keep):
    pairs = ((p_held, p_got), (q_held, q_got))
    for half, (held, got) in enumerate(pairs):
        keep[half, :, :first], keep[half, :, first:] = joined(held.at[0], got, 0, first)


def close_body(first, held, *refs):
    pieces = []
    for half in range(held.shape[0]):
        one, two = held[half, :, :first], held[half, :, first:]
        for got in refs[:-1]:
            more = unpack(got, half, first, held.shape[2])
            one, two = one + more[0], two + more[1]
        pieces.append((one, two))
    pack(refs[-1], pieces)


def spread_body(first, me, *refs):
    one, two = refs[-2:]
    width = first + two.shape[1]
    narrow = digit(me, 1, len(refs[:-2]))
    for place, ref in enumerate(refs[:-2]):
        rows = ref.shape[1]
        for half in range(2):
            at = half * (one.shape[0] // 2) + (narrow ^ place) * rows
            at = pl.ds(pl.multiple_of(at, rows), rows)
            one[at, :], two[at, :] = unpack(ref, half, first, width)


def from_behind(block, axis, distance):
    devices = range(lax.axis_size(axis))
    route = [((i - distance) % len(devices), i) for i in devices]
    return lax.ppermute(block, axis, route)


def swapped(block, axis, bit):
    return lax.ppermute(block, axis, [(i, i ^ bit) for i in range(lax.axis_size(axis))])


def bits(count):
    return [1 << b for b in range(count.bit_length() - 1)]


def shards(inputs, w_first, w_second, requests, slots, counts, edge_weight, offsets):
    rows = inputs.shape[0]
    width = w_second.shape[1]
    peers = lax.axis_size("wide")
    group = lax.axis_size("narrow")
    din, hid = w_first.shape
    total_rows = rows * peers * group
    powers = peers & (peers - 1) == 0 and group & (group - 1) == 0 and peers > 1 and group > 1
    assert powers, "axis sizes"
    me = lax.axis_index(("wide", "narrow")).reshape(1).astype(jnp.int32)
    count = 4 if hid % (4 * LANES) == 0 else 1
    hidden, codes, sent = pl.pallas_call(
        forward_body,
        out_shape=(
            jax.ShapeDtypeStruct((rows, hid), BF16),
            jax.ShapeDtypeStruct((rows, width), F32),
            jax.ShapeDtypeStruct((rows, width), BF16),
        ),
        in_specs=[SMEM] + [pl.BlockSpec(memory_space=pltpu.HBM)] * 3,
        out_specs=[VMEM] * 3,
        scratch_shapes=[
            pltpu.VMEM(inputs.shape, BF16),
            pltpu.VMEM((count, din, hid // count), BF16),
            pltpu.VMEM(w_second.shape, BF16),
            pltpu.SemaphoreType.DMA((count + 2,)),
        ],
        compiler_params=pltpu.CompilerParams(vmem_limit_bytes=16 * 1024 * 1024),
    )(me, *(pltpu.with_memory_space_constraint(a, pltpu.HBM) for a in (inputs, w_first, w_second)))
    steps = offsets.shape[0]
    paired = steps == 4
    if paired:
        two = from_behind(sent, "narrow", 2)
        own = swapped(sent, "narrow", 1)
        four = from_behind(two, "narrow", 2)
        pair = swapped(two, "narrow", 1)
        three = lax.ppermute(two, "narrow", [((n - 1) % group, n) for n in range(0, group, 2)])
        blocks = [(pair, own), (two,), (three, pair), (four,)]
        order = [1, 0, 3, 2]
    else:
        blocks = []
        for step in range(steps):
            source = sent if step < 2 else blocks[step - 2][0]
            blocks.append((from_behind(source, "narrow", min(step, 1) + 1),))
        order = list(range(steps))
    near = [sent]
    for bit in bits(peers):
        near += [swapped(block, "wide", bit) for block in near]
    inputs_t, hidden_t = call(
        flip_body,
        (jax.ShapeDtypeStruct((din, rows), BF16), jax.ShapeDtypeStruct((hid, rows), BF16)),
        0,
        2,
    )(inputs, hidden)
    size = peers * requests.shape[1]
    weight = call(
        weight_body,
        jax.ShapeDtypeStruct((rows, size), BF16),
        0,
        3,
        [pltpu.VMEM((size, rows), BF16)],
    )(slots.T, counts[None], edge_weight.T)
    like = jax.ShapeDtypeStruct(codes.shape, F32)
    twice = twice_of(rows, width)

    def far(step, grad):
        given = blocks[step] + (() if grad is None else (grad,))
        body = functools.partial(far_body, step, len(blocks[step]))
        return call(body, like, 2, 1 + len(given), [twice])(me, offsets, codes, *given)

    grad = far(order[0], None)
    grad = call(functools.partial(near_body, group), like, 1, 4 + len(near), [pltpu.VMEM((size, width), BF16)])(
        me, codes, requests, weight, grad, *near
    )
    for step in order[1:-1]:
        grad = far(step, grad)
    step = order[-1]
    last_inputs = (me, offsets, codes, *blocks[step], grad, w_second, hidden, inputs_t, hidden_t)
    scale = 2.0 / (slots.shape[1] * math.sqrt(total_rows))
    chunk = din // (peers * group)
    scratch = [twice, pltpu.VMEM((rows, width), BF16), pltpu.VMEM((rows, hid), BF16)]
    if din != hid or chunk % 32 or din % (peers * group) or peers < 4 or not 4 <= group <= LANES // SHARE or width % LANES:
        one, two = call(
            functools.partial(last_plain_body, step, scale),
            (jax.ShapeDtypeStruct((din, hid), F32), jax.ShapeDtypeStruct((hid, width), F32)),
            2,
            len(last_inputs) - 2,
            scratch,
        )(*last_inputs)
        owned = (
            lax.psum_scatter(one, "wide", scatter_dimension=0, tiled=True),
            lax.psum_scatter(two, "wide", scatter_dimension=0, tiled=True),
        )
        return lax.psum(owned, "narrow")

    first, full = hid, hid + width

    def plain(*shape):
        return jax.ShapeDtypeStruct((*shape, full), F32)

    def coded(*shape):
        return jax.ShapeDtypeStruct((*shape, full + LANES), I16)

    keep = got = None
    for bit in bits(peers)[:-1]:
        below = bit * group
        groups, lines = peers // (2 * bit), din // peers
        if keep is None:
            send, dcodes, dpre = call(
                functools.partial(give_body, step, scale, below),
                (
                    coded(groups, lines),
                    jax.ShapeDtypeStruct((rows, width), BF16),
                    jax.ShapeDtypeStruct((rows, hid), BF16),
                ),
                2,
                len(last_inputs) - 2,
                [twice],
            )(*last_inputs)
            keep = call(functools.partial(hold_body, below), plain(groups, lines), 1, 4)(me, dcodes, dpre, inputs_t, hidden_t)
        else:
            keep, send = call(
                functools.partial(stage_body, first, below), (plain(groups, lines), coded(groups, lines)), 1, 2
            )(me, keep.reshape(groups, 2, lines, full), got.reshape(groups, 2, lines, full + LANES))
        got = swapped(send, "wide", bit)
    last, lines, others = peers // 2, chunk // 2, group // 2
    below = last * group

    def message(count):
        return jax.ShapeDtypeStruct((count * (full // LANES) + 1, lines, LANES), I16)

    def do(body, shapes, scalars, arrays):
        return call(body, shapes, len(scalars), len(arrays))(*scalars, *arrays)

    rest = (
        keep.reshape(2, 2, others, 2, lines, full),
        got.reshape(2, 2, others, 2, lines, full + LANES),
    )
    sends = [
        do(functools.partial(part_send_body, first, below, half), message(2 * others), (me,), rest)
        for half in range(2)
    ]
    p_keep, q_keep = do(
        functools.partial(part_keep_body, first, below), (plain(others, 2, lines), plain(2, others, lines)), (me,), rest
    )
    p_got, q_got = swapped(sends[0], "wide", last), swapped(sends[1], "narrow", 1)
    rest = (p_keep, q_keep, p_got, q_got)
    p_send, q_send = do(functools.partial(cross_send_body, first), (message(others),) * 2, (), rest)
    p_keep, q_keep = do(functools.partial(cross_keep_body, first), (plain(others, lines),) * 2, (), rest)
    p_got, q_got = swapped(p_send, "narrow", 1), swapped(q_send, "wide", last)
    rest = (p_keep, q_keep, p_got, q_got)
    sends = do(functools.partial(deal_send_body, first), (message(2),) * (others - 1), (), rest)
    keep = do(functools.partial(deal_keep_body, first), plain(2, lines), (), rest)
    gots = [swapped(send, "narrow", 2 * k) for k, send in enumerate(sends, 1)]
    mine = do(functools.partial(close_body, first), message(2), (), (keep, *gots))
    pieces = [mine] + [swapped(mine, "narrow", k) for k in range(1, group)]
    return do(
        functools.partial(spread_body, first),
        (
            jax.ShapeDtypeStruct((din // peers, hid), F32),
            jax.ShapeDtypeStruct((hid // peers, width), F32),
        ),
        (me,),
        pieces,
    )


def solution(mesh):
    return jax.shard_map(
        shards,
        mesh=mesh,
        in_specs=(
            P(("wide", "narrow"), None),
            P(),
            P(),
            P(("wide", "narrow"), None),
            P(("wide", "narrow"), None),
            P(("wide", "narrow")),
            P(("wide", "narrow"), None),
            P(),
        ),
        out_specs=(P("wide", None), P("wide", None)),
        check_vma=False,
    )
```

```python
import functools
import math

import jax
import jax.numpy as jnp
from jax import lax
from jax.experimental import pallas as pl
from jax.experimental.pallas import tpu as pltpu
from jax.sharding import PartitionSpec as P


NEGW = 8
TILE = 128
PACK = 16
SHARE = 16
LANES = 128
HALF = LANES // 2
FULL = 32000.0
STEPS = 128.0
TINY = 1e-30

F32 = jnp.float32
BF16 = jnp.bfloat16
I16 = jnp.int16
VMEM = pl.BlockSpec(memory_space=pltpu.VMEM)
SMEM = pl.BlockSpec(memory_space=pltpu.SMEM)


def digit(me, below, count):
    return lax.rem(lax.div(me[0], below), count)


def call(body, out_shape, n_scalars, n_arrays, scratch=(), mib=16):
    many = isinstance(out_shape, (list, tuple))
    return pl.pallas_call(
        body,
        out_shape=out_shape,
        in_specs=[SMEM] * n_scalars + [VMEM] * n_arrays,
        out_specs=[VMEM] * len(out_shape) if many else VMEM,
        scratch_shapes=list(scratch),
        compiler_params=pltpu.CompilerParams(vmem_limit_bytes=mib * 1024 * 1024),
    )


def dot(a, b):
    return lax.dot_general(a, b, (((1,), (0,)), ((), ())), preferred_element_type=F32)


def dot_nt(a, b):
    return lax.dot_general(a, b, (((1,), (1,)), ((), ())), preferred_element_type=F32)


def parts(value, count):
    out = []
    for _ in range(count):
        part = value.astype(BF16)
        out.append(part)
        value = value - part.astype(F32)
    return out


def distances(y, z):
    rows = y.shape[0]
    gram = dot_nt(jnp.concatenate(parts(y, 3), axis=0), z)
    gram = gram[:rows] + gram[rows : 2 * rows] + gram[2 * rows :]
    zf = z.astype(F32)
    z_norm = jnp.broadcast_to(jnp.sum(zf * zf, axis=1, keepdims=True), (z.shape[0], rows)).T
    y_norm = jnp.sum(y * y, axis=1, keepdims=True)
    return jnp.maximum(y_norm + z_norm - 2.0 * gram, 0.0) * (1.0 / z.shape[1])


def pull(y, z, coef):
    rows = y.shape[0]
    high, low = parts(coef, 2)
    total = jnp.sum(high.astype(F32) + low.astype(F32), axis=1, keepdims=True)
    mixed = dot(jnp.concatenate([high, low], axis=0), z)
    return y * total - (mixed[:rows] + mixed[rows:])


def forward_body(me, inputs, w_first, w_second, hidden, codes, sent, block, first, second, sems):
    del me
    count = first.shape[0]
    size = first.shape[2]
    copies = [pltpu.make_async_copy(inputs, block, sems.at[0])]
    for c in range(count):
        columns = w_first.at[:, c * size : (c + 1) * size]
        copies.append(pltpu.make_async_copy(columns, first.at[c], sems.at[c + 1]))
    copies.append(pltpu.make_async_copy(w_second, second, sems.at[count + 1]))
    for copy in copies:
        copy.start()
    copies[0].wait()
    for c in range(count):
        copies[c + 1].wait()
        columns = slice(c * size, (c + 1) * size)
        hidden[:, columns] = jnp.maximum(dot(block[...], first[c]), 0.0).astype(BF16)
    copies[-1].wait()
    value = dot(hidden[...], second[...])
    codes[...] = value
    sent[...] = value.astype(BF16)


def flip_body(inputs, hidden, inputs_t, hidden_t):
    inputs_t[...] = inputs[...].T
    hidden_t[...] = hidden[...].T


def weight_body(slots, counts, edges, out, total):
    tile = 32
    rows = slots.shape[1]
    for at in range(0, out.shape[1], tile):
        place = at + lax.broadcasted_iota(jnp.int32, (tile, rows), 0)
        weight = jnp.zeros((tile, rows), F32)
        for k in range(slots.shape[0]):
            live = jnp.where(k < counts[...], edges[k : k + 1, :].astype(F32), 0.0)
            weight = weight + jnp.where(place == slots[k : k + 1, :], live, 0.0)
        total[at : at + tile, :] = weight.astype(BF16)
    out[...] = total[...].T


def near_body(group, me, codes, requests, weight, grad, *rest):
    out, table = rest[-2:]
    cap = requests.shape[1]
    wide = digit(me, group, len(rest[:-2]))
    for place, block in enumerate(rest[:-2]):
        asked = requests[pl.ds(wide ^ place, 1), :]
        hot = lax.broadcasted_iota(jnp.int32, (block.shape[0], cap), 0) == asked
        hot = jnp.where(hot, 1.0, 0.0).astype(BF16).T
        at = pl.ds(pl.multiple_of((wide ^ place) * cap, cap), cap)
        table[at, :] = dot(hot, block[...]).astype(BF16)
    tile = min(codes.shape[0], TILE)
    part = 2 * tile
    for at in range(0, codes.shape[0], tile):
        rows_of = slice(at, at + tile)
        y = codes[rows_of, :]
        total = grad[rows_of, :]
        for low in range(0, table.shape[0], part):
            z = table[low : low + part, :]
            strength = weight[rows_of, low : low + part].astype(F32)
            total = total + pull(y, z, strength / (1.0 + distances(y, z)))
        out[rows_of, :] = total


def repulsion(me, codes, choices, offset, twice, put):
    rows = codes.shape[0]
    block = choices[0][...]
    if len(choices) > 1:
        block = jnp.where(digit(me, 1, 2) > 0, choices[1][...], block)
    tile = min(rows, TILE)
    window = tile + max(tile, LANES)
    for at in range(0, twice.shape[0], rows):
        end = min(rows, twice.shape[0] - at)
        twice[at : at + end, :] = block[:end, :]
    start = (offset // PACK) * PACK
    shape = (tile, window)
    place = lax.broadcasted_iota(jnp.int32, shape, 1) - lax.broadcasted_iota(jnp.int32, shape, 0)
    place = place - (offset - start)
    band = (place >= 0) & (place < NEGW)
    for at in range(0, rows, tile):
        y = codes[at : at + tile, :]
        z = twice[pl.ds(pl.multiple_of(start + at, PACK), window), :]
        dist = distances(y, z)
        onep = 1.0 + dist
        coef = jnp.where(band, 1.0 / (onep * (dist + 0.1 * onep)), 0.0)
        put(slice(at, at + tile), pull(y, z, coef))


def twice_of(rows, width):
    tile = min(rows, TILE)
    return pltpu.VMEM((2 * rows + max(tile, LANES), width), BF16)


def far_body(step, count, me, offsets, codes, *rest):
    choices, rest = rest[:count], rest[count:]
    out, twice = rest[-2:]
    grad = rest[0] if len(rest) > 2 else None

    def put(at, value):
        out[at, :] = -value if grad is None else grad[at, :] - value

    repulsion(me, codes, choices, offsets[step], twice, put)


def encode(one, two):
    quanta, codes = [], []
    for piece in (one, two):
        top = jnp.maximum(jnp.max(jnp.abs(piece), axis=1, keepdims=True), TINY)
        code = jnp.ceil(jnp.log2(top) * STEPS)
        quanta.append(short(jnp.round(piece * (FULL * jnp.exp2(code * (-1.0 / STEPS))))))
        codes.append(code)
    return quanta, codes


def short(value):
    return value.astype(jnp.int32).astype(I16)


def unit_of(code):
    return jnp.exp2(code * (1.0 / STEPS)) * (1.0 / FULL)


def pack(ref, pieces):
    rows = ref.shape[1]
    lane = lax.broadcasted_iota(jnp.int32, (rows, LANES), 1)
    header = jnp.zeros((rows, LANES), F32)
    at = 0
    for k, piece in enumerate(pieces):
        quanta, codes = encode(*piece)
        for quantum in quanta:
            for column in range(0, quantum.shape[1], LANES):
                ref[at] = quantum[:, column : column + LANES]
                at += 1
        for j, code in enumerate(codes):
            header = jnp.where(lane >= SHARE * k + SHARE // 2 * j, code, header)
    ref[at] = short(header)


def unpack(ref, k, first, width):
    tiles = width // LANES
    header = ref[ref.shape[0] - 1].astype(jnp.int32).astype(F32)
    out = []
    for j, (low, high) in enumerate(((0, first // LANES), (first // LANES, tiles))):
        lane = SHARE * k + SHARE // 2 * j
        unit = unit_of(header[:, lane : lane + 1])
        value = [ref[k * tiles + g].astype(jnp.int32).astype(F32) for g in range(low, high)]
        out.append(jnp.concatenate(value, axis=1) * unit)
    return out


def decode(packed, first, width):
    code = packed[:, width:].astype(jnp.int32).astype(F32)
    out = []
    for lane, low, high in ((0, 0, first), (HALF, first, width)):
        unit = unit_of(code[:, lane : lane + 1])
        out.append(packed[:, low:high].astype(jnp.int32).astype(F32) * unit)
    return out


def put_encoded(ref, one, two):
    first, width = one.shape[1], one.shape[1] + two.shape[1]
    (ref[:, :first], ref[:, first:width]), codes = encode(one, two)
    lane = lax.broadcasted_iota(jnp.int32, (one.shape[0], LANES), 1)
    ref[:, width:] = short(jnp.where(lane < HALF, codes[0], codes[1]))


def gradients(step, scale, me, offsets, codes, choices, grad, w_second, hidden, twice, dcodes, dpre):
    def put(at, value):
        dcodes[at, :] = (scale * (grad[at, :] - value)).astype(BF16)

    repulsion(me, codes, choices, offsets[step], twice, put)
    size = 2 * LANES
    for at in range(0, hidden.shape[1], size):
        columns = slice(at, at + size)
        wide = dot_nt(dcodes[...], w_second[columns, :])
        dpre[:, columns] = jnp.where(hidden[:, columns] > 0, wide, 0.0).astype(BF16)


def give_body(step, scale, below, me, offsets, codes, *rest):
    *choices, grad, w_second, hidden, inputs_t, hidden_t, send, dcodes, dpre, twice = rest
    gradients(step, scale, me, offsets, codes, choices, grad, w_second, hidden, twice, dcodes, dpre)
    groups, rows = send.shape[:2]
    one, two = halves(1 - digit(me, below, 2), groups, rows, dcodes, dpre, inputs_t, hidden_t)
    for a in range(groups):
        at = slice(a * rows, (a + 1) * rows)
        put_encoded(send.at[a], one[at], two[at])


def hold_body(below, me, dcodes, dpre, inputs_t, hidden_t, keep):
    groups, rows = keep.shape[:2]
    first = dpre.shape[1]
    one, two = halves(digit(me, below, 2), groups, rows, dcodes, dpre, inputs_t, hidden_t)
    for a in range(groups):
        at = slice(a * rows, (a + 1) * rows)
        keep[a, :, :first], keep[a, :, first:] = one[at], two[at]


def halves(side, groups, rows, dcodes, dpre, inputs_t, hidden_t):
    def taken(ref):
        at = [pl.ds(pl.multiple_of((2 * a + side) * rows, rows), rows) for a in range(groups)]
        return jnp.concatenate([ref[rows_of, :] for rows_of in at], axis=0)

    return dot(taken(inputs_t), dpre[...]), dot(taken(hidden_t), dcodes[...])


def last_plain_body(step, scale, me, offsets, codes, *rest):
    *choices, grad, w_second, hidden, inputs_t, hidden_t, one, two, twice, dcodes, dpre = rest
    gradients(step, scale, me, offsets, codes, choices, grad, w_second, hidden, twice, dcodes, dpre)
    one[...] = dot(inputs_t[...], dpre[...])
    two[...] = dot(hidden_t[...], dcodes[...])


def summed(held, got, first):
    one, two = decode(got, first, held.shape[-1])
    return held[:, :first] + one, held[:, first:] + two


def stage_body(first, below, me, held, got, keep, send):
    mine = digit(me, below, 2)
    for a in range(held.shape[0]):
        put_encoded(send.at[a], *summed(held.at[a, 1 - mine], got.at[a, 1 - mine], first))
    for a in range(held.shape[0]):
        keep[a, :, :first], keep[a, :, first:] = summed(held.at[a, mine], got.at[a, mine], first)


def part_index(below, me, others):
    mine, here, place = digit(me, below, 2), digit(me, 1, 2), digit(me, 2, others)

    def p_at(side, k, r):
        return (mine ^ side, 0, place ^ k, here ^ r)

    def q_at(side, r, k):
        return (mine ^ r, 1, place ^ k, here ^ side)

    return p_at, q_at


def part_send_body(first, below, half, me, held, got, send):
    others = held.shape[2]
    index = part_index(below, me, others)[half]
    pairs = [(i, j) for i in range((others, 2)[half]) for j in range((2, others)[half])]
    pack(send, [summed(held.at[index(1, *pair)], got.at[index(1, *pair)], first) for pair in pairs])


def part_keep_body(first, below, me, held, got, p_keep, q_keep):
    others = held.shape[2]
    p_at, q_at = part_index(below, me, others)
    for k in range(others):
        for r in range(2):
            at = p_at(0, k, r)
            p_keep[k, r, :, :first], p_keep[k, r, :, first:] = summed(held.at[at], got.at[at], first)
            at = q_at(0, r, k)
            q_keep[r, k, :, :first], q_keep[r, k, :, first:] = summed(held.at[at], got.at[at], first)


def joined(held, got, k, first):
    one, two = unpack(got, k, first, held.shape[-1])
    return held[:, :first] + one, held[:, first:] + two


def cross_send_body(first, p_held, q_held, p_got, q_got, p_send, q_send):
    others = p_held.shape[0]
    pack(p_send, [joined(p_held.at[k, 1], p_got, 2 * k + 1, first) for k in range(others)])
    pack(q_send, [joined(q_held.at[1, k], q_got, others + k, first) for k in range(others)])


def cross_keep_body(first, p_held, q_held, p_got, q_got, p_keep, q_keep):
    for k in range(p_held.shape[0]):
        p_keep[k, :, :first], p_keep[k, :, first:] = joined(p_held.at[k, 0], p_got, 2 * k, first)
        q_keep[k, :, :first], q_keep[k, :, first:] = joined(q_held.at[0, k], q_got, k, first)


def deal_send_body(first, p_held, q_held, p_got, q_got, *sends):
    pairs = ((p_held, p_got), (q_held, q_got))
    for k, send in enumerate(sends, 1):
        pack(send, [joined(held.at[k], got, k, first) for held, got in pairs])


def deal_keep_body(first, p_held, q_held, p_got, q_got, keep):
    pairs = ((p_held, p_got), (q_held, q_got))
    for half, (held, got) in enumerate(pairs):
        keep[half, :, :first], keep[half, :, first:] = joined(held.at[0], got, 0, first)


def close_body(first, held, *refs):
    pieces = []
    for half in range(held.shape[0]):
        one, two = held[half, :, :first], held[half, :, first:]
        for got in refs[:-1]:
            more = unpack(got, half, first, held.shape[2])
            one, two = one + more[0], two + more[1]
        pieces.append((one, two))
    pack(refs[-1], pieces)


def spread_body(first, me, *refs):
    one, two = refs[-2:]
    width = first + two.shape[1]
    narrow = digit(me, 1, len(refs[:-2]))
    for place, ref in enumerate(refs[:-2]):
        rows = ref.shape[1]
        for half in range(2):
            at = half * (one.shape[0] // 2) + (narrow ^ place) * rows
            at = pl.ds(pl.multiple_of(at, rows), rows)
            one[at, :], two[at, :] = unpack(ref, half, first, width)


def from_behind(block, axis, distance):
    devices = range(lax.axis_size(axis))
    route = [((i - distance) % len(devices), i) for i in devices]
    return lax.ppermute(block, axis, route)


def swapped(block, axis, bit):
    return lax.ppermute(block, axis, [(i, i ^ bit) for i in range(lax.axis_size(axis))])


def bits(count):
    return [1 << b for b in range(count.bit_length() - 1)]


def shards(inputs, w_first, w_second, requests, slots, counts, edge_weight, offsets):
    rows = inputs.shape[0]
    width = w_second.shape[1]
    peers = lax.axis_size("wide")
    group = lax.axis_size("narrow")
    din, hid = w_first.shape
    total_rows = rows * peers * group
    powers = peers & (peers - 1) == 0 and group & (group - 1) == 0 and peers > 1 and group > 1
    assert powers, "axis sizes"
    me = lax.axis_index(("wide", "narrow")).reshape(1).astype(jnp.int32)
    count = 2 if hid % (2 * LANES) == 0 else 1
    hidden, codes, sent = pl.pallas_call(
        forward_body,
        out_shape=(
            jax.ShapeDtypeStruct((rows, hid), BF16),
            jax.ShapeDtypeStruct((rows, width), F32),
            jax.ShapeDtypeStruct((rows, width), BF16),
        ),
        in_specs=[SMEM] + [pl.BlockSpec(memory_space=pltpu.HBM)] * 3,
        out_specs=[VMEM] * 3,
        scratch_shapes=[
            pltpu.VMEM(inputs.shape, BF16),
            pltpu.VMEM((count, din, hid // count), BF16),
            pltpu.VMEM(w_second.shape, BF16),
            pltpu.SemaphoreType.DMA((count + 2,)),
        ],
        compiler_params=pltpu.CompilerParams(vmem_limit_bytes=16 * 1024 * 1024),
    )(me, *(pltpu.with_memory_space_constraint(a, pltpu.HBM) for a in (inputs, w_first, w_second)))
    steps = offsets.shape[0]
    paired = steps == 4
    if paired:
        two = from_behind(sent, "narrow", 2)
        own = swapped(sent, "narrow", 1)
        four = from_behind(two, "narrow", 2)
        pair = swapped(two, "narrow", 1)
        three = lax.ppermute(two, "narrow", [((n - 1) % group, n) for n in range(0, group, 2)])
        blocks = [(pair, own), (two,), (three, pair), (four,)]
        order = [1, 0, 3, 2]
    else:
        blocks = []
        for step in range(steps):
            source = sent if step < 2 else blocks[step - 2][0]
            blocks.append((from_behind(source, "narrow", min(step, 1) + 1),))
        order = list(range(steps))
    near = [sent]
    for bit in bits(peers):
        near += [swapped(block, "wide", bit) for block in near]
    inputs_t, hidden_t = call(
        flip_body,
        (jax.ShapeDtypeStruct((din, rows), BF16), jax.ShapeDtypeStruct((hid, rows), BF16)),
        0,
        2,
    )(inputs, hidden)
    size = peers * requests.shape[1]
    weight = call(
        weight_body,
        jax.ShapeDtypeStruct((rows, size), BF16),
        0,
        3,
        [pltpu.VMEM((size, rows), BF16)],
    )(slots.T, counts[None], edge_weight.T)
    like = jax.ShapeDtypeStruct(codes.shape, F32)
    twice = twice_of(rows, width)

    def far(step, grad):
        given = blocks[step] + (() if grad is None else (grad,))
        body = functools.partial(far_body, step, len(blocks[step]))
        return call(body, like, 2, 1 + len(given), [twice])(me, offsets, codes, *given)

    grad = far(order[0], None)
    grad = call(functools.partial(near_body, group), like, 1, 4 + len(near), [pltpu.VMEM((size, width), BF16)])(
        me, codes, requests, weight, grad, *near
    )
    for step in order[1:-1]:
        grad = far(step, grad)
    step = order[-1]
    last_inputs = (me, offsets, codes, *blocks[step], grad, w_second, hidden, inputs_t, hidden_t)
    scale = 2.0 / (slots.shape[1] * math.sqrt(total_rows))
    chunk = din // (peers * group)
    scratch = [twice, pltpu.VMEM((rows, width), BF16), pltpu.VMEM((rows, hid), BF16)]
    if din != hid or chunk % 32 or din % (peers * group) or peers < 4 or not 4 <= group <= LANES // SHARE or width % LANES:
        one, two = call(
            functools.partial(last_plain_body, step, scale),
            (jax.ShapeDtypeStruct((din, hid), F32), jax.ShapeDtypeStruct((hid, width), F32)),
            2,
            len(last_inputs) - 2,
            scratch,
        )(*last_inputs)
        owned = (
            lax.psum_scatter(one, "wide", scatter_dimension=0, tiled=True),
            lax.psum_scatter(two, "wide", scatter_dimension=0, tiled=True),
        )
        return lax.psum(owned, "narrow")

    first, full = hid, hid + width

    def plain(*shape):
        return jax.ShapeDtypeStruct((*shape, full), F32)

    def coded(*shape):
        return jax.ShapeDtypeStruct((*shape, full + LANES), I16)

    keep = got = None
    for bit in bits(peers)[:-1]:
        below = bit * group
        groups, lines = peers // (2 * bit), din // peers
        if keep is None:
            send, dcodes, dpre = call(
                functools.partial(give_body, step, scale, below),
                (
                    coded(groups, lines),
                    jax.ShapeDtypeStruct((rows, width), BF16),
                    jax.ShapeDtypeStruct((rows, hid), BF16),
                ),
                2,
                len(last_inputs) - 2,
                [twice],
            )(*last_inputs)
            keep = call(functools.partial(hold_body, below), plain(groups, lines), 1, 4)(me, dcodes, dpre, inputs_t, hidden_t)
        else:
            keep, send = call(
                functools.partial(stage_body, first, below), (plain(groups, lines), coded(groups, lines)), 1, 2
            )(me, keep.reshape(groups, 2, lines, full), got.reshape(groups, 2, lines, full + LANES))
        got = swapped(send, "wide", bit)
    last, lines, others = peers // 2, chunk // 2, group // 2
    below = last * group

    def message(count):
        return jax.ShapeDtypeStruct((count * (full // LANES) + 1, lines, LANES), I16)

    def do(body, shapes, scalars, arrays):
        return call(body, shapes, len(scalars), len(arrays))(*scalars, *arrays)

    rest = (
        keep.reshape(2, 2, others, 2, lines, full),
        got.reshape(2, 2, others, 2, lines, full + LANES),
    )
    sends = [
        do(functools.partial(part_send_body, first, below, half), message(2 * others), (me,), rest)
        for half in range(2)
    ]
    p_keep, q_keep = do(
        functools.partial(part_keep_body, first, below), (plain(others, 2, lines), plain(2, others, lines)), (me,), rest
    )
    p_got, q_got = swapped(sends[0], "wide", last), swapped(sends[1], "narrow", 1)
    rest = (p_keep, q_keep, p_got, q_got)
    p_send, q_send = do(functools.partial(cross_send_body, first), (message(others),) * 2, (), rest)
    p_keep, q_keep = do(functools.partial(cross_keep_body, first), (plain(others, lines),) * 2, (), rest)
    p_got, q_got = swapped(p_send, "narrow", 1), swapped(q_send, "wide", last)
    rest = (p_keep, q_keep, p_got, q_got)
    sends = do(functools.partial(deal_send_body, first), (message(2),) * (others - 1), (), rest)
    keep = do(functools.partial(deal_keep_body, first), plain(2, lines), (), rest)
    gots = [swapped(send, "narrow", 2 * k) for k, send in enumerate(sends, 1)]
    mine = do(functools.partial(close_body, first), message(2), (), (keep, *gots))
    held = {0: mine}
    for k in range(1, group):
        relayed = k % 2 == 1 and k > 3
        held[k] = swapped(held[k - 1] if relayed else mine, "narrow", 1 if relayed else k)
    pieces = [held[k] for k in range(group)]
    return do(
        functools.partial(spread_body, first),
        (
            jax.ShapeDtypeStruct((din // peers, hid), F32),
            jax.ShapeDtypeStruct((hid // peers, width), F32),
        ),
        (me,),
        pieces,
    )


def solution(mesh):
    return jax.shard_map(
        shards,
        mesh=mesh,
        in_specs=(
            P(("wide", "narrow"), None),
            P(),
            P(),
            P(("wide", "narrow"), None),
            P(("wide", "narrow"), None),
            P(("wide", "narrow")),
            P(("wide", "narrow"), None),
            P(),
        ),
        out_specs=(P("wide", None), P("wide", None)),
        check_vma=False,
    )
```
